256 devices in a mesh: dp: 32 (over z, x), mp: 8 (over y, core).
Axes of the slice: x: 4, y: 4, z: 8, core: 2. Of those that a mesh axis runs over, the one named last changes fastest.
Arguments:
- activations: bfloat16 [16384, 3072], P('dp', 'mp'), may hold values from -6 to 6
- out_grads: bfloat16 [16384, 6144], P('dp', 'mp'), may hold values from -0.25 to 0.25
- error: bfloat16 [32, 3072, 6144], P('dp', 'mp'), may hold values from -8 to 8
- sketch: bfloat16 [6144, 64], replicated, may hold values from -0.078125 to 0.078125
- momentum: float32 [3072, 6144], P('mp', 'dp'), may hold values from -6 to 6
Outputs:
- error_new: bfloat16 [32, 3072, 6144], P('dp', 'mp')
- momentum_new: float32 [3072, 6144], P('mp', 'dp')
- next_sketch: bfloat16 [6144, 64], replicated
The draws below stay inside these ranges and needn't reach their ends.
All inputs are finite; a program needn't handle non-finite values.
Results may differ from the reference program's by a relative error of at most 0.0057.
Values may be sent and summed in bfloat16 or wider, within the bound.
No kernel may reach another device: no remote copies, remote signals or barrier semaphores. Data moves between devices by JAX's collectives and lax.ppermute only.
A program may use at most 64 MiB of HBM per device.

```python
import jax
import jax.numpy as jnp
from jax import lax

D = 6144
ROWS = 3072
RANK = 64
TOK_DEV = 512
WORKERS = 32
TOKENS = 16384


def draw_error(key, part):
    shared = jax.random.normal(jax.random.fold_in(key, 11), (ROWS, D), jnp.float32)
    single = jax.random.normal(jax.random.fold_in(key, 12), (WORKERS, ROWS, D), jnp.float32)
    values = 0.8 * shared + 0.6 * single
    return jnp.clip(values, -8.0, 8.0).astype(jnp.bfloat16)


def steps_of(key, extent, pieces, smallest, largest):
    def one(axis_at, blocks):
        draws = jax.random.uniform(jax.random.fold_in(jax.random.fold_in(key, 6), axis_at), (blocks,), jnp.float32, smallest / len(pieces), largest / len(pieces))
        return jnp.repeat(jnp.exp(draws), extent[axis_at] // blocks).reshape((-1,) + (1,) * (len(extent) - axis_at - 1))

    gain = one(*pieces[0])
    for cut in pieces[1:]:
        gain = gain * one(*cut)
    return gain


def noise(rng, shape, spread, reach, shards=(), held_as=jnp.bfloat16):
    loudness = steps_of(rng, shape, shards, -0.22, 0.18) if shards else 1.0
    array = jax.random.normal(rng, shape, jnp.float32) * spread * loudness
    return jnp.minimum(jnp.maximum(array, -reach), reach).astype(held_as)


def setup_inputs(seed: int = 0) -> dict:
    seeds = jax.random.split(jax.random.key(seed), 6)
    return {
        "activations": noise(seeds[0], (TOKENS, ROWS), 1.0, 6.0, ((0, 32), (1, 8))),
        "out_grads": noise(seeds[1], (TOKENS, D), TOK_DEV ** -0.5, 0.25, ((0, 32), (1, 8))),
        "error": draw_error(jax.random.fold_in(seeds[5], 71), 0),
        "sketch": noise(seeds[3], (D, RANK), D ** -0.5, 0.078125),
        "momentum": noise(seeds[4], (ROWS, D), 1.0, 6.0, ((0, 8), (1, 32)), jnp.float32),
    }


beta_decay = 0.9

def reference(activations, out_grads, error, sketch, momentum):
    inputs = activations.reshape(WORKERS, TOK_DEV, ROWS)
    grads = out_grads.reshape(WORKERS, TOK_DEV, D)

    def feed_one(items):
        inputs_w, grads_w, error_w = items
        product = lax.dot_general(inputs_w.astype(jnp.float32), grads_w.astype(jnp.float32), (((0,), (0,)), ((), ())), preferred_element_type=jnp.float32)
        return (product + error_w.astype(jnp.float32)).astype(jnp.bfloat16)
    accumulated = lax.map(feed_one, (inputs, grads, error))

    def left_step(total, fed_w):
        return (total + jnp.dot(fed_w.astype(jnp.float32), sketch.astype(jnp.float32), preferred_element_type=jnp.float32), None)
    left_sketch = lax.scan(left_step, jnp.zeros((ROWS, RANK), jnp.float32), accumulated)[0]
    gram_matrix = jnp.dot(left_sketch.T.astype(jnp.float32), left_sketch.astype(jnp.float32), precision=lax.Precision.HIGHEST, preferred_element_type=jnp.float32)
    factor = jnp.linalg.cholesky(gram_matrix)
    basis_rows = jax.scipy.linalg.solve_triangular(factor, left_sketch.T, lower=True).T.astype(jnp.bfloat16)

    def right_step(total, fed_w):
        term = lax.dot_general(fed_w.astype(jnp.float32), basis_rows.astype(jnp.float32), (((0,), (0,)), ((), ())), preferred_element_type=jnp.float32)
        return (total + term, None)
    right_sketch = lax.scan(right_step, jnp.zeros((D, RANK), jnp.float32), accumulated)[0]
    next_sketch = right_sketch.astype(jnp.bfloat16)
    decoded = lax.dot_general(basis_rows.astype(jnp.float32), next_sketch.astype(jnp.float32), (((1,), (1,)), ((), ())), preferred_element_type=jnp.float32)
    momentum_new = beta_decay * momentum + decoded

    def error_one(fed_w):
        return (fed_w.astype(jnp.float32) - decoded / WORKERS).astype(jnp.bfloat16)
    error_new = lax.map(error_one, accumulated)
    return (error_new, momentum_new, next_sketch)
```

```python
import jax
import jax.numpy as jnp
from jax import lax
from jax.experimental import pallas as pl
from jax.experimental.pallas import tpu as pltpu
from jax.sharding import Mesh
from jax.sharding import PartitionSpec as P

DP = ("dp_0", "dp_1")
YY = "mp_0"
CC = "mp_1"
F32 = jnp.float32
BF16 = jnp.bfloat16
HIGHEST = lax.Precision.HIGHEST
D, RANK, ROWS, TOK, COLS, WORKERS = 6144, 64, 384, 512, 768, 32
INTERPRET = False
BETA = 0.9

NN = (((1,), (0,)), ((), ()))
NT = (((1,), (1,)), ((), ()))


def dot(a, b, dims=NN, precision=None):
    return lax.dot_general(a, b, dims, precision=precision, preferred_element_type=F32)


def two_terms(x):
    high = x.astype(BF16)
    low = (x - high.astype(F32)).astype(BF16)
    return jnp.concatenate([high, low], axis=0)


def halves_added(x):
    return x[: x.shape[0] // 2] + x[x.shape[0] // 2 :]


def call(body, out_shape, name, flops, **kw):
    return pl.pallas_call(
        body,
        out_shape=out_shape,
        name=name,
        interpret=INTERPRET,
        cost_estimate=pl.CostEstimate(flops=flops, bytes_accessed=1 << 20, transcendentals=0),
        **kw,
    )


def sds(shape, dtype):
    return jax.ShapeDtypeStruct(shape, dtype)


def grads_sketch_body(ids, grads, sketch, out):
    out[...] = dot(grads[...], sketch[...]).T


def grads_sketch(ids, grads, sketch):
    spec = pltpu.PrefetchScalarGridSpec(
        num_scalar_prefetch=1,
        grid=(1,),
        in_specs=[
            pl.BlockSpec((TOK, COLS), lambda i, s: (0, 0)),
            pl.BlockSpec((COLS, RANK), lambda i, s: (s[0], 0)),
        ],
        out_specs=pl.BlockSpec((RANK, TOK), lambda i, s: (0, 0)),
    )
    return call(grads_sketch_body, sds((RANK, TOK), F32), "grads_sketch", 10**8, grid_spec=spec)(
        ids, grads, sketch
    )


def error_sketch_body(error, sketch, out, acc):
    step = pl.program_id(0)

    @pl.when(step == 0)
    def _():
        acc[...] = jnp.zeros_like(acc)

    acc[...] += dot(error[...], sketch[...])

    @pl.when(step == pl.num_programs(0) - 1)
    def _():
        out[...] = acc[...].T


def error_sketch(error, sketch):
    width = 1536
    return call(
        error_sketch_body,
        sds((RANK, ROWS), F32),
        "error_sketch",
        3 * 10**9,
        grid=(D // width,),
        in_specs=[
            pl.BlockSpec((ROWS, width), lambda i: (0, i)),
            pl.BlockSpec((width, RANK), lambda i: (i, 0)),
        ],
        out_specs=pl.BlockSpec((RANK, ROWS), lambda i: (0, 0)),
        scratch_shapes=[pltpu.VMEM((ROWS, RANK), F32)],
    )(error, sketch)


def left_term_body(own, one, two, three, acts, from_error, out):
    total = own[...] + one[...].astype(F32) + two[...].astype(F32) + three[...].astype(F32)
    left = halves_added(dot(two_terms(total), acts[...])) + from_error[...]
    for r in range(8):
        for j in range(3):
            out[4 * r + j] = left[8 * r : 8 * r + 8, 128 * j : 128 * j + 128]
        out[4 * r + 3] = jnp.zeros((8, 128), F32)


def left_term(own, parts, acts, from_error):
    return call(left_term_body, sds((WORKERS, 8, 128), F32), "left_term", 10**8)(
        own, *parts, acts, from_error
    )


def sum_and_copy_body(arrived, out):
    total = jnp.sum(arrived[...].astype(F32), axis=0).astype(out.dtype)
    out[...] = jnp.broadcast_to(total[None], out.shape)


def sum_and_copy(arrived, dtype, name):
    return call(sum_and_copy_body, sds(arrived.shape, dtype), name, 10**7)(arrived)


def left_products_body(tiles, acts, left_out, left_terms, acts_left_terms, gram):
    rows = [
        jnp.concatenate([tiles[4 * r + j] for j in range(3)], axis=1) for r in range(8)
    ]
    left = jnp.concatenate(rows, axis=0)
    left_out[...] = left
    terms = two_terms(left)
    left_terms[...] = terms
    acts_left_terms[...] = two_terms(halves_added(dot(terms, acts[...], NT)))
    gram[...] = dot(left, left, NT, HIGHEST)


def left_products(tiles, acts):
    return call(
        left_products_body,
        (
            sds((RANK, ROWS), F32),
            sds((2 * RANK, ROWS), BF16),
            sds((2 * RANK, TOK), BF16),
            sds((RANK, RANK), F32),
        ),
        "left_products",
        10**8,
    )(tiles, acts)


def columns(block):
    return pl.ds(pl.multiple_of(block * COLS, COLS), COLS)


def copies_of_grads(pieces, place, sems, first):
    own, up, half_a, half_b, down = pieces
    h = TOK // 2
    return [
        [pltpu.make_async_copy(own, place.at[0], sems.at[first])],
        [pltpu.make_async_copy(up, place.at[1], sems.at[first + 1])],
        [
            pltpu.make_async_copy(half_a, place.at[2, pl.ds(0, h)], sems.at[first + 2]),
            pltpu.make_async_copy(half_b, place.at[2, pl.ds(h, h)], sems.at[first + 3]),
        ],
        [pltpu.make_async_copy(down, place.at[3], sems.at[first + 4])],
    ]


def right_terms_body(
    ids, left_terms, acts_left_terms, error, g0, g1, g2a, g2b, g3, out, held_g, held_e, sems
):
    grads = copies_of_grads((g0, g1, g2a, g2b, g3), held_g, sems, 0)
    errors = [
        pltpu.make_async_copy(error.at[:, columns(ids[k])], held_e.at[k], sems.at[5 + k])
        for k in range(4)
    ]
    for k in range(4):
        errors[k].start()
        for c in grads[k]:
            c.start()
    for k in (0, 1, 3, 2):
        errors[k].wait()
        term = dot(left_terms[...], held_e[k])
        for c in grads[k]:
            c.wait()
        out[k] = halves_added(term + dot(acts_left_terms[...], held_g[k]))


def right_terms(ids, left_terms, acts_left_terms, error, grads, name):
    any_ = pl.BlockSpec(memory_space=pl.ANY)
    vmem = pl.BlockSpec(memory_space=pltpu.VMEM)
    return call(
        right_terms_body,
        sds((4, RANK, COLS), F32),
        name,
        3 * 10**9,
        in_specs=[pl.BlockSpec(memory_space=pltpu.SMEM), vmem, vmem, any_] + [any_] * 5,
        out_specs=vmem,
        scratch_shapes=[
            pltpu.VMEM((4, TOK, COLS), BF16),
            pltpu.VMEM((4, ROWS, COLS), BF16),
            pltpu.SemaphoreType.DMA((9,)),
        ],
    )(ids, left_terms, acts_left_terms, error, *grads)


def add_blocks_body(a, b, o0, o1, o2, o3):
    for k, o in enumerate((o0, o1, o2, o3)):
        o[...] = a[k] + b[k]


def add_blocks(a, b):
    return call(add_blocks_body, (sds((RANK, COLS), F32),) * 4, "add_blocks", 10**8)(a, b)


def factor_body(own, one, two, three, left, inverse_out, basis_out):
    gram = own[...] + one[...] + two[...] + three[...]
    lanes = lax.broadcasted_iota(jnp.int32, (RANK, RANK), 1)
    subs = lax.broadcasted_iota(jnp.int32, (RANK, RANK), 0)
    eye = jnp.where(lanes == subs, 1.0, 0.0).astype(F32)
    work = jnp.concatenate([gram, eye], axis=1)
    rows = lax.broadcasted_iota(jnp.int32, (RANK, 2 * RANK), 0)
    for j in range(RANK - 1):
        row = work[j : j + 1, :]
        ratio = work[:, j : j + 1] / work[j : j + 1, j : j + 1]
        work = work - jnp.where(rows > j, ratio * row, 0.0)
    pivots = jnp.sum(jnp.where(lanes == subs, work[:, :RANK], 0.0), axis=1, keepdims=True)
    inverse = work[:, RANK:] / jnp.sqrt(pivots)
    inverse_out[...] = inverse
    basis_out[...] = dot(inverse, left[...], NN, HIGHEST).T.astype(BF16)


def factor(own, parts, left):
    return call(
        factor_body, (sds((RANK, RANK), F32), sds((ROWS, RANK), BF16)), "factor", 6 * 10**9
    )(own, *parts, left)


def right_term_body(inverse, own, one, two, three, out):
    total = own[...] + one[...] + two[...] + three[...]
    right = dot(inverse[...], total, NN, HIGHEST)
    for j in range(6):
        for r in range(4):
            out[4 * j + r] = right[16 * r : 16 * r + 16, 128 * j : 128 * j + 128].astype(out.dtype)
    out[24:] = jnp.zeros((8, 16, 128), out.dtype)


def right_term(inverse, own, parts):
    return call(right_term_body, sds((WORKERS, 16, 128), F32), "right_term", 10**8)(
        inverse, own, *parts
    )


def fed_body(ids, acts, error, *rest):
    grads, out = rest[:10], rest[10]
    held_g, held_e, held_o, sems, out_sems = rest[11:]
    copies = copies_of_grads(grads[:5], held_g.at[pl.ds(0, 4)], sems, 0) + copies_of_grads(
        grads[5:], held_g.at[pl.ds(4, 4)], sems, 5
    )
    errors = [
        pltpu.make_async_copy(error.at[:, columns(ids[k])], held_e.at[k], sems.at[10 + k])
        for k in range(8)
    ]
    for k in range(8):
        errors[k].start()
        for c in copies[k]:
            c.start()
    turned = acts[...].T
    stores = []
    for k in range(8):
        errors[k].wait()
        for c in copies[k]:
            c.wait()
        held_o[k] = (dot(turned, held_g[k]) + held_e[k].astype(F32)).astype(BF16)
        store = pltpu.make_async_copy(held_o.at[k], out.at[:, columns(ids[k])], out_sems.at[k])
        store.start()
        stores.append(store)
    for store in stores:
        store.wait()


def fed_of(ids, acts, error, grads):
    any_ = pl.BlockSpec(memory_space=pl.ANY)
    vmem = pl.BlockSpec(memory_space=pltpu.VMEM)
    return call(
        fed_body,
        sds((ROWS, D), BF16),
        "fed",
        6 * 10**9,
        in_specs=[pl.BlockSpec(memory_space=pltpu.SMEM), vmem, any_] + [any_] * 10,
        out_specs=any_,
        scratch_shapes=[
            pltpu.VMEM((8, TOK, COLS), BF16),
            pltpu.VMEM((8, ROWS, COLS), BF16),
            pltpu.VMEM((8, ROWS, COLS), BF16),
            pltpu.SemaphoreType.DMA((18,)),
            pltpu.SemaphoreType.DMA((8,)),
        ],
    )(ids, acts, error, *grads)


def outputs_body(ids, fed, basis, *rest):
    blocks, momentum = rest[:8], rest[8]
    error_new, momentum_new, next_sketch, turned = rest[9:]
    step = pl.program_id(0)
    for k in range(8):

        @pl.when(step == k)
        def _():
            for j in range(6):
                for r in range(4):
                    turned[16 * r : 16 * r + 16, 128 * j : 128 * j + 128] = blocks[k][4 * j + r]

    decoded = dot(basis[...], turned[...])
    error_new[0] = (fed[...].astype(F32) - decoded / WORKERS).astype(BF16)
    next_sketch[...] = turned[...].astype(F32).T.astype(BF16)

    @pl.when(ids[step] == ids[8])
    def _():
        first = pl.multiple_of(ids[9] * 192, 64)
        part = next_sketch[pl.ds(first, 192), :]
        momentum_new[...] = BETA * momentum[...] + dot(basis[...], part, NT)


def outputs(ids, fed, basis, blocks, momentum):
    spec = pltpu.PrefetchScalarGridSpec(
        num_scalar_prefetch=1,
        grid=(8,),
        in_specs=[
            pl.BlockSpec((ROWS, COLS), lambda i, s: (0, s[i])),
            pl.BlockSpec((ROWS, RANK), lambda i, s: (0, 0)),
        ]
        + [pl.BlockSpec((24, 16, 128), lambda i, s: (0, 0, 0))] * 8
        + [pl.BlockSpec((ROWS, 192), lambda i, s: (0, 0))],
        out_specs=[
            pl.BlockSpec((1, ROWS, COLS), lambda i, s: (0, 0, s[i])),
            pl.BlockSpec((ROWS, 192), lambda i, s: (0, 0)),
            pl.BlockSpec((COLS, RANK), lambda i, s: (s[i], 0)),
        ],
        scratch_shapes=[pltpu.VMEM((RANK, COLS), BF16)],
    )
    return call(
        outputs_body,
        (sds((1, ROWS, D), BF16), sds((ROWS, 192), F32), sds((D, RANK), BF16)),
        "outputs",
        10**9,
        grid_spec=spec,
    )(ids, fed, basis, *blocks, momentum)


def along_y(x, k):
    return lax.ppermute(x, YY, [(i, (i + k) % 4) for i in range(4)])


def other_core(x):
    return lax.ppermute(x, CC, [(0, 1), (1, 0)])


def to_workers(x):
    return lax.all_to_all(x, DP, split_axis=0, concat_axis=0, tiled=True)


def three_along_y(x):
    return [along_y(x, k) for k in (1, 2, 3)]


def after(x, *others):
    return lax.optimization_barrier((x, *others))[0]


def local(activations, out_grads, error, sketch, momentum):
    own_error = error[0]
    y, c = lax.axis_index(YY), lax.axis_index(CC)
    w = lax.axis_index(DP)
    near = [2 * ((y + k) % 4) + c for k in range(4)]
    far = [2 * ((y + k) % 4) + 1 - c for k in range(4)]
    ids = jnp.stack(near + far + [w // 4, w % 4]).astype(jnp.int32)

    with jax.named_scope("grads_sketch"):
        mine = grads_sketch(ids, out_grads, sketch)
        pair = mine + other_core(mine)
        others = three_along_y(pair.astype(BF16))
    from_error = error_sketch(own_error, sketch)
    tiles = left_term(pair, others, activations, from_error)

    with jax.named_scope("gather_one"):
        held = after(out_grads, *others)
        g3 = along_y(held, 1)
        g1 = along_y(held, -1)
        p0 = other_core(held)

    with jax.named_scope("left_sum"):
        arrived = to_workers(tiles)
    copies = sum_and_copy(arrived, F32, "left_sum")
    with jax.named_scope("gather_two"):
        g1, g3 = lax.optimization_barrier((g1, g3, copies))[:2]
        half = TOK // 2
        g2a = along_y(g1[:half], -1)
        g2b = along_y(g3[half:], 1)
        p1 = other_core(g1)
        p3 = other_core(g3)
    with jax.named_scope("left_copies"):
        tiles = to_workers(copies)
    with jax.named_scope("gather_three"):
        p2a = other_core(g2a)
        p2b = other_core(g2b)

    left, left_terms, acts_left_terms, gram = left_products(tiles, activations)
    with jax.named_scope("gram"):
        gram_pair = gram + other_core(gram)
        gram_parts = three_along_y(gram_pair)
    near_g = (out_grads, g1, g2a, g2b, g3)
    far_g = (p0, p1, p2a, p2b, p3)
    send = right_terms(ids[4:8], left_terms, acts_left_terms, own_error, far_g, "right_far")
    with jax.named_scope("right_core"):
        got = other_core(send)
    keep = right_terms(ids[0:4], left_terms, acts_left_terms, own_error, near_g, "right_near")
    q = add_blocks(keep, got)
    with jax.named_scope("right_y"):
        parts = [along_y(q[k], k) for k in (1, 2, 3)]
    inverse, basis = factor(gram_pair, gram_parts, left)
    fed = fed_of(ids[:8], activations, own_error, near_g + far_g)
    pieces = right_term(inverse, q[0], parts)
    with jax.named_scope("right_sum"):
        arrived = to_workers(pieces)
    copies = sum_and_copy(arrived, BF16, "right_sum")
    with jax.named_scope("right_copies"):
        block = to_workers(copies)[:24]
    with jax.named_scope("spread"):
        n3 = along_y(block, 1)
        n2 = along_y(block, 2)
        n1 = along_y(block, -1)
        near_n = (block, n1, n2, n3)
        far_n = tuple(other_core(n) for n in near_n)
    return outputs(ids, fed, basis, near_n + far_n, momentum)


def solution(mesh):
    split = Mesh(mesh.devices.reshape(8, 4, 4, 2), (*DP, YY, CC))
    mp = (YY, CC)
    return jax.shard_map(
        local,
        mesh=split,
        in_specs=(P(DP, mp), P(DP, mp), P(DP, mp, None), P(), P(mp, DP)),
        out_specs=(P(DP, mp, None), P(mp, DP), P()),
        check_vma=False,
    )
```

```python
import jax
import jax.numpy as jnp
from jax import lax
from jax.experimental import pallas as pl
from jax.experimental.pallas import tpu as pltpu
from jax.sharding import Mesh
from jax.sharding import PartitionSpec as P


DP = ("dp_0", "dp_1")
YY = "mp_0"
CC = "mp_1"
F32 = jnp.float32
BF16 = jnp.bfloat16
HIGHEST = lax.Precision.HIGHEST
D, RANK, ROWS, TOK, COLS, WORKERS = 6144, 64, 384, 512, 768, 32
INTERPRET = False
BETA = 0.9

NN = (((1,), (0,)), ((), ()))
NT = (((1,), (1,)), ((), ()))


def dot(a, b, dims=NN, precision=None):
    return lax.dot_general(a, b, dims, precision=precision, preferred_element_type=F32)


def two_terms(x):
    high = x.astype(BF16)
    low = (x - high.astype(F32)).astype(BF16)
    return jnp.concatenate([high, low], axis=0)


def halves_added(x):
    return x[: x.shape[0] // 2] + x[x.shape[0] // 2 :]


def call(body, out_shape, flops, **kw):
    return pl.pallas_call(
        body,
        out_shape=out_shape,
        interpret=INTERPRET,
        cost_estimate=pl.CostEstimate(flops=flops, bytes_accessed=1 << 20, transcendentals=0),
        **kw,
    )


def sds(shape, dtype):
    return jax.ShapeDtypeStruct(shape, dtype)


VMEM = pl.BlockSpec(memory_space=pltpu.VMEM)
HBM = pl.BlockSpec(memory_space=pltpu.HBM)


def block_at(ahead, other):
    y, c = lax.axis_index(YY), lax.axis_index(CC)
    return 2 * lax.rem(y + ahead, 4) + (1 - c if other else c)


def columns(block):
    return pl.ds(pl.multiple_of(block * COLS, COLS), COLS)


def grads_sketch_body(grads, sketch_t, out, held, sem):
    cut = pltpu.make_async_copy(sketch_t.at[:, columns(block_at(0, False))], held, sem)
    cut.start()
    cut.wait()
    out[...] = dot(held[...], grads[...], NT)


def grads_sketch(grads, sketch_t):
    return call(
        grads_sketch_body,
        sds((RANK, TOK), F32),
        10**8,
        in_specs=[VMEM, HBM],
        out_specs=VMEM,
        scratch_shapes=[pltpu.VMEM((RANK, COLS), BF16), pltpu.SemaphoreType.DMA(())],
    )(grads, sketch_t)


def pair_body(a, b, out, rounded):
    total = a[...] + b[...]
    out[...] = total
    rounded[...] = total.astype(BF16)


def pair_sum(a, b):
    return call(pair_body, (sds(a.shape, F32), sds(a.shape, BF16)), 10**7)(a, b)


def error_sketch_body(error, sketch_t, out, held, sems):
    parts = 8
    width = D // parts
    copies = [
        pltpu.make_async_copy(error.at[:, pl.ds(k * width, width)], held.at[k], sems.at[k])
        for k in range(parts)
    ]
    for c in copies:
        c.start()
    acc = jnp.zeros((RANK, ROWS), F32)
    for k in range(parts):
        copies[k].wait()
        acc = acc + dot(sketch_t[:, k * width : (k + 1) * width], held[k], NT)
    out[...] = acc


def error_sketch(error, sketch_t):
    return call(
        error_sketch_body,
        sds((RANK, ROWS), F32),
        3 * 10**9,
        in_specs=[HBM, VMEM],
        out_specs=VMEM,
        scratch_shapes=[pltpu.VMEM((8, ROWS, D // 8), BF16), pltpu.SemaphoreType.DMA((8,))],
    )(error, sketch_t)


def left_term_body(own, one, two, three, acts, from_error, out):
    total = own[...] + one[...].astype(F32) + two[...].astype(F32) + three[...].astype(F32)
    left = halves_added(dot(two_terms(total), acts[...])) + from_error[...]
    for r in range(8):
        for j in range(3):
            out[4 * r + j] = left[8 * r : 8 * r + 8, 128 * j : 128 * j + 128]
        out[4 * r + 3] = jnp.zeros((8, 128), F32)


def left_term(own, parts, acts, from_error):
    return call(left_term_body, sds((WORKERS, 8, 128), F32), 10**8)(own, *parts, acts, from_error)


def sum_and_copy_body(arrived, out):
    total = jnp.sum(arrived[...].astype(F32), axis=0).astype(out.dtype)
    out[...] = jnp.broadcast_to(total[None], out.shape)


def sum_and_copy(arrived, dtype):
    return call(sum_and_copy_body, sds(arrived.shape, dtype), 10**7)(arrived)


def left_products_body(tiles, acts, left_out, left_terms, small):
    rows = [jnp.concatenate([tiles[4 * r + j] for j in range(3)], axis=1) for r in range(8)]
    left = jnp.concatenate(rows, axis=0)
    left_out[...] = left
    terms = two_terms(left)
    left_terms[...] = terms
    small[:, :TOK] = halves_added(dot(terms, acts[...], NT))
    gram = dot(left, left, NT, HIGHEST)
    small[:, TOK:] = jnp.concatenate([gram, jnp.zeros_like(gram)], axis=1)


def left_products(tiles, acts):
    return call(
        left_products_body,
        (
            sds((RANK, ROWS), F32),
            sds((2 * RANK, ROWS), BF16),
            sds((RANK, TOK + 128), F32),
        ),
        10**8,
    )(tiles, acts)


def right_blocks(other, left_terms, error, held, sems, store):
    copies = [
        pltpu.make_async_copy(error.at[:, columns(block_at(k, other))], held.at[k], sems.at[k])
        for k in range(4)
    ]
    for c in copies:
        c.start()
    for k in range(4):
        copies[k].wait()
        store(k, halves_added(dot(left_terms[...], held[k])))


def right_far_body(left_terms, error, out, held, sems):
    def store(k, block):
        out[k] = block

    right_blocks(True, left_terms, error, held, sems, store)


def right_near_body(left_terms, error, got, o0, o1, o2, o3, held, sems):
    outs = (o0, o1, o2, o3)

    def store(k, block):
        outs[k][...] = block + got[k]

    right_blocks(False, left_terms, error, held, sems, store)


RIGHT_SCRATCH = [pltpu.VMEM((4, ROWS, COLS), BF16), pltpu.SemaphoreType.DMA((4,))]


def right_far(left_terms, error):
    return call(
        right_far_body,
        sds((4, RANK, COLS), F32),
        10**9,
        in_specs=[VMEM, HBM],
        out_specs=VMEM,
        scratch_shapes=RIGHT_SCRATCH,
    )(left_terms, error)


def right_near(left_terms, error, got):
    return call(
        right_near_body,
        (sds((RANK, COLS), F32),) * 4,
        10**9,
        in_specs=[VMEM, HBM, VMEM],
        out_specs=(VMEM,) * 4,
        scratch_shapes=RIGHT_SCRATCH,
    )(left_terms, error, got)


def factor_body(own, one, two, three, left, inverse_out, basis_out, acts_left):
    small = own[...] + one[...] + two[...] + three[...]
    acts_left[...] = two_terms(small[:, :TOK])
    lanes = lax.broadcasted_iota(jnp.int32, (RANK, RANK), 1)
    subs = lax.broadcasted_iota(jnp.int32, (RANK, RANK), 0)
    eye = jnp.where(lanes == subs, 1.0, 0.0).astype(F32)
    work = jnp.concatenate([small[:, TOK : TOK + RANK], eye], axis=1)
    rows = lax.broadcasted_iota(jnp.int32, (RANK, 2 * RANK), 0)
    for j in range(RANK - 1):
        row = work[j : j + 1, :]
        ratio = work[:, j : j + 1] / work[j : j + 1, j : j + 1]
        work = work - jnp.where(rows > j, ratio * row, 0.0)
    pivots = jnp.sum(jnp.where(lanes == subs, work[:, :RANK], 0.0), axis=1, keepdims=True)
    inverse = work[:, RANK:] / jnp.sqrt(pivots)
    inverse_out[...] = inverse
    basis_out[...] = dot(inverse, left[...], NN, HIGHEST).T.astype(BF16)


def factor(own, parts, left):
    return call(
        factor_body,
        (sds((RANK, RANK), F32), sds((ROWS, RANK), BF16), sds((2 * RANK, TOK), BF16)),
        6 * 10**9,
    )(own, *parts, left)


def right_term_body(inverse, acts_left, grads, own, one, two, three, out):
    total = own[...] + one[...] + two[...] + three[...]
    total = total + halves_added(dot(acts_left[...], grads[...]))
    right = dot(inverse[...], total, NN, HIGHEST)
    for j in range(6):
        for r in range(4):
            out[4 * j + r] = right[16 * r : 16 * r + 16, 128 * j : 128 * j + 128].astype(out.dtype)
    out[24:] = jnp.zeros((8, 16, 128), out.dtype)


def right_term(inverse, acts_left, grads, own, parts):
    return call(right_term_body, sds((WORKERS, 16, 128), BF16), 10**8)(
        inverse, acts_left, grads, own, *parts
    )


def fed_body(acts, error, *rest):
    grads, out = rest[:8], rest[8]
    held_g, held_e, sems = rest[9:]
    loads = [
        pltpu.make_async_copy(grads[k], held_g.at[k], sems.at[k]) for k in range(8)
    ]
    errors = [
        pltpu.make_async_copy(
            error.at[:, columns(block_at(k % 4, k >= 4))], held_e.at[k], sems.at[8 + k]
        )
        for k in range(8)
    ]
    for k in range(8):
        errors[k].start()
        loads[k].start()
    turned = acts[...].T
    for k in range(8):
        errors[k].wait()
        loads[k].wait()
        out[k] = (dot(turned, held_g[k]) + held_e[k].astype(F32)).astype(BF16)


def fed_of(acts, error, grads):
    return call(
        fed_body,
        sds((8, ROWS, COLS), BF16),
        6 * 10**9,
        in_specs=[VMEM, HBM] + [HBM] * 8,
        out_specs=VMEM,
        scratch_shapes=[
            pltpu.VMEM((8, TOK, COLS), BF16),
            pltpu.VMEM((8, ROWS, COLS), BF16),
            pltpu.SemaphoreType.DMA((16,)),
        ],
    )(acts, error, *grads)


def outputs_body(fed, basis, *rest):
    blocks, momentum_t = rest[:8], rest[8]
    error_new, momentum_new_t, sketch_t = rest[9:12]
    held, turned, sems = rest[12:]
    w = lax.axis_index(DP)
    stores = []
    for k in range(8):
        where = block_at(k % 4, k >= 4)
        rows = [
            jnp.concatenate([blocks[k][4 * j + r] for j in range(6)], axis=1) for r in range(4)
        ]
        block = jnp.concatenate(rows, axis=0)
        decoded = dot(basis[...], block)
        held[k] = (fed[k].astype(F32) - decoded / WORKERS).astype(BF16)
        store = pltpu.make_async_copy(held.at[k], error_new.at[0, :, columns(where)], sems.at[k])
        store.start()
        stores.append(store)
        sketch_t[:, columns(where)] = block

        @pl.when(where == w // 4)
        def _():
            turned[...] = block.astype(F32).T
            first = pl.multiple_of(lax.rem(w, 4) * 192, 64)
            part = turned[pl.ds(first, 192), :].astype(BF16)
            momentum_new_t[...] = BETA * momentum_t[...] + dot(part, basis[...], NT)

    for store in stores:
        store.wait()


def outputs(fed, basis, blocks, momentum_t):
    return call(
        outputs_body,
        (sds((1, ROWS, D), BF16), sds((192, ROWS), F32), sds((RANK, D), BF16)),
        10**9,
        in_specs=[VMEM] * 11,
        out_specs=(HBM, VMEM, VMEM),
        scratch_shapes=[
            pltpu.VMEM((8, ROWS, COLS), BF16),
            pltpu.VMEM((COLS, RANK), F32),
            pltpu.SemaphoreType.DMA((8,)),
        ],
    )(fed, basis, *blocks, momentum_t)


def along_y(x, k):
    return lax.ppermute(x, YY, [(i, (i + k) % 4) for i in range(4)])


def other_core(x):
    return lax.ppermute(x, CC, [(0, 1), (1, 0)])


def to_workers(x):
    return lax.all_to_all(x, DP, split_axis=0, concat_axis=0, tiled=True)


def after(x, *others):
    return lax.optimization_barrier((x, *others))[0]


def step(activations, out_grads, error, sketch, momentum):
    own_error = error[0]
    sketch_t = sketch.T

    mine = grads_sketch(out_grads, sketch_t)
    pair, rounded = pair_sum(mine, other_core(mine))
    others = []
    for k in (1, 2, 3):
        others.append(along_y(rounded, k))
    from_error = error_sketch(own_error, sketch_t)
    tiles = left_term(pair, others, activations, from_error)

    held = after(out_grads, *others)
    gathered = []
    for k in (1, 2, 3):
        gathered.append(along_y(held, -k % 4))

    arrived = to_workers(tiles)
    copies = sum_and_copy(arrived, F32)
    tiles = to_workers(copies)

    left, left_terms, small = left_products(tiles, activations)
    small = small + other_core(small)
    small_parts = [along_y(small, k) for k in (1, 2, 3)]
    send = right_far(left_terms, own_error)
    got = other_core(send)
    q = right_near(left_terms, own_error, got)
    parts = [along_y(q[k], k) for k in (1, 2, 3)]
    inverse, basis, acts_left = factor(small, small_parts, left)
    pieces = right_term(inverse, acts_left, out_grads, q[0], parts)

    near_g = (out_grads, *gathered)
    far_g = []
    for k in range(4):
        far_g.append(other_core(after(near_g[k], pieces)))
    arrived = to_workers(pieces)
    copies = sum_and_copy(arrived, BF16)
    fed = fed_of(activations, own_error, (*near_g, *far_g))
    block = to_workers(copies)[:24]
    n3, n2, n1 = along_y(block, 1), along_y(block, 2), along_y(block, -1)
    near_n = (block, n1, n2, n3)
    far_n = tuple(other_core(n) for n in near_n)
    error_new, momentum_t, sketch_t = outputs(fed, basis, near_n + far_n, momentum.T)
    return error_new, momentum_t.T, sketch_t.T


def solution(mesh):
    split = Mesh(mesh.devices.reshape(8, 4, 4, 2), (*DP, YY, CC))
    mp = (YY, CC)
    return jax.shard_map(
        step,
        mesh=split,
        in_specs=(P(DP, mp), P(DP, mp), P(DP, mp, None), P(), P(mp, DP)),
        out_specs=(P(DP, mp, None), P(mp, DP), P()),
        check_vma=False,
    )
```

```python
import jax
import jax.numpy as jnp
from jax import lax
from jax.experimental import pallas as pl
from jax.experimental.pallas import tpu as pltpu
from jax.sharding import Mesh
from jax.sharding import PartitionSpec as P


DP = ("dp_0", "dp_1")
YY = "mp_0"
CC = "mp_1"
F32 = jnp.float32
BF16 = jnp.bfloat16
HIGHEST = lax.Precision.HIGHEST
D, RANK, ROWS, TOK, COLS, WORKERS = 6144, 64, 384, 512, 768, 32
INTERPRET = False
BETA = 0.9

NN = (((1,), (0,)), ((), ()))
NT = (((1,), (1,)), ((), ()))


def dot(a, b, dims=NN, precision=None):
    return lax.dot_general(a, b, dims, precision=precision, preferred_element_type=F32)


def two_terms(x):
    high = x.astype(BF16)
    low = (x - high.astype(F32)).astype(BF16)
    return jnp.concatenate([high, low], axis=0)


def halves_added(x):
    return x[: x.shape[0] // 2] + x[x.shape[0] // 2 :]


def call(body, out_shape, flops, mib=8, **kw):
    return pl.pallas_call(
        body,
        out_shape=out_shape,
        interpret=INTERPRET,
        compiler_params=pltpu.CompilerParams(vmem_limit_bytes=mib << 20),
        cost_estimate=pl.CostEstimate(flops=flops, bytes_accessed=1 << 20, transcendentals=0),
        **kw,
    )


def sds(shape, dtype):
    return jax.ShapeDtypeStruct(shape, dtype)


def on_chip(shape, dtype):
    return pltpu.VMEM(shape, dtype)


VMEM = pl.BlockSpec(memory_space=pltpu.VMEM)
HBM = pl.BlockSpec(memory_space=pltpu.HBM)


def block_at(ahead, other):
    y, c = lax.axis_index(YY), lax.axis_index(CC)
    return 2 * lax.rem(y + ahead, 4) + (1 - c if other else c)


def columns(block):
    return pl.ds(pl.multiple_of(block * COLS, COLS), COLS)


def grads_sketch_body(grads, sketch_t, out, held, sem):
    cut = pltpu.make_async_copy(sketch_t.at[:, columns(block_at(0, False))], held, sem)
    cut.start()
    cut.wait()
    out[...] = dot(held[...], grads[...], NT)


def grads_sketch(grads, sketch_t):
    return call(
        grads_sketch_body,
        on_chip((RANK, TOK), F32),
        10**8,
        in_specs=[VMEM, HBM],
        out_specs=VMEM,
        scratch_shapes=[pltpu.VMEM((RANK, COLS), BF16), pltpu.SemaphoreType.DMA(())],
    )(grads, sketch_t)


def pair_body(a, b, out, rounded):
    total = a[...] + b[...]
    out[...] = total
    rounded[...] = total.astype(BF16)


def pair_sum(a, b):
    return call(pair_body, (on_chip(a.shape, F32), on_chip(a.shape, BF16)), 10**7)(a, b)


def error_sketch_body(error, sketch_t, out, held, sems):
    places = [columns(block_at(k % 4, k >= 4)) for k in range(8)]
    copies = [
        pltpu.make_async_copy(error.at[:, places[k]], held.at[k], sems.at[k]) for k in range(8)
    ]
    for c in copies:
        c.start()
    acc = jnp.zeros((RANK, ROWS), F32)
    for k in range(8):
        copies[k].wait()
        acc = acc + dot(sketch_t[:, places[k]], held[k], NT)
    out[...] = acc


def error_sketch(error, sketch_t):
    return call(
        error_sketch_body,
        (on_chip((RANK, ROWS), F32), on_chip((8, ROWS, COLS), BF16)),
        3 * 10**9,
        in_specs=[HBM, VMEM],
        out_specs=(VMEM, VMEM),
        scratch_shapes=[pltpu.SemaphoreType.DMA((8,))],
    )(error, sketch_t)


def left_term_body(own, one, two, three, acts, from_error, out):
    total = own[...] + one[...].astype(F32) + two[...].astype(F32) + three[...].astype(F32)
    left = halves_added(dot(two_terms(total), acts[...])) + from_error[...]
    for r in range(8):
        for j in range(3):
            out[4 * r + j] = left[8 * r : 8 * r + 8, 128 * j : 128 * j + 128]
        out[4 * r + 3] = jnp.zeros((8, 128), F32)


def left_term(own, parts, acts, from_error):
    return call(left_term_body, on_chip((WORKERS, 8, 128), F32), 10**8)(
        own, *parts, acts, from_error
    )


def sum_and_copy_body(arrived, out):
    total = jnp.sum(arrived[...].astype(F32), axis=0).astype(out.dtype)
    out[...] = jnp.broadcast_to(total[None], out.shape)


def sum_and_copy(arrived, dtype):
    return call(sum_and_copy_body, on_chip(arrived.shape, dtype), 10**7)(arrived)


def left_products_body(tiles, acts, left_out, left_terms, small):
    rows = [jnp.concatenate([tiles[4 * r + j] for j in range(3)], axis=1) for r in range(8)]
    left = jnp.concatenate(rows, axis=0)
    left_out[...] = left
    terms = two_terms(left)
    left_terms[...] = terms
    small[:, :TOK] = halves_added(dot(terms, acts[...], NT))
    gram = dot(left, left, NT, HIGHEST)
    small[:, TOK:] = jnp.concatenate([gram, jnp.zeros_like(gram)], axis=1)


def left_products(tiles, acts):
    return call(
        left_products_body,
        (
            on_chip((RANK, ROWS), F32),
            on_chip((2 * RANK, ROWS), BF16),
            on_chip((RANK, TOK + 128), F32),
        ),
        10**8,
    )(tiles, acts)


def right_far_body(left_terms, error, out):
    for k in range(4):
        out[k] = halves_added(dot(left_terms[...], error[4 + k]))


def right_near_body(left_terms, error, got, out):
    y = lax.axis_index(YY)
    for k in range(4):
        out[lax.rem(y + k, 4)] = halves_added(dot(left_terms[...], error[k])) + got[k]


def right_far(left_terms, error):
    shape = on_chip((4, RANK, COLS), F32)
    return call(right_far_body, shape, 10**9)(left_terms, error)


def right_near(left_terms, error, got):
    shape = on_chip((4, RANK, COLS), F32)
    return call(right_near_body, shape, 10**9)(left_terms, error, got)


def factor_body(own, one, two, three, left, inverse_out, basis_out, acts_left):
    small = own[...] + one[...] + two[...] + three[...]
    acts_left[...] = two_terms(small[:, :TOK])
    lanes = lax.broadcasted_iota(jnp.int32, (RANK, RANK), 1)
    subs = lax.broadcasted_iota(jnp.int32, (RANK, RANK), 0)
    eye = jnp.where(lanes == subs, 1.0, 0.0).astype(F32)
    work = jnp.concatenate([small[:, TOK : TOK + RANK], eye], axis=1)
    rows = lax.broadcasted_iota(jnp.int32, (RANK, 2 * RANK), 0)
    for j in range(RANK - 1):
        row = work[j : j + 1, :]
        ratio = work[:, j : j + 1] / work[j : j + 1, j : j + 1]
        work = work - jnp.where(rows > j, ratio * row, 0.0)
    pivots = jnp.sum(jnp.where(lanes == subs, work[:, :RANK], 0.0), axis=1, keepdims=True)
    inverse = work[:, RANK:] / jnp.sqrt(pivots)
    inverse_out[...] = inverse
    basis_out[...] = dot(inverse, left[...], NN, HIGHEST).T.astype(BF16)


def factor(own, parts, left):
    return call(
        factor_body,
        (on_chip((RANK, RANK), F32), on_chip((ROWS, RANK), BF16), on_chip((2 * RANK, TOK), BF16)),
        6 * 10**9,
    )(own, *parts, left)


def right_term_body(inverse, acts_left, grads, terms, out):
    total = terms[0] + terms[1] + terms[2] + terms[3]
    total = total + halves_added(dot(acts_left[...], grads[...]))
    right = dot(inverse[...], total, NN, HIGHEST)
    for j in range(6):
        for r in range(4):
            out[4 * j + r] = right[16 * r : 16 * r + 16, 128 * j : 128 * j + 128].astype(out.dtype)
    out[24:] = jnp.zeros((8, 16, 128), out.dtype)


def right_term(inverse, acts_left, grads, terms):
    return call(right_term_body, on_chip((WORKERS, 16, 128), BF16), 10**8)(
        inverse, acts_left, grads, terms
    )


def fed_body(acts, error, *rest):
    grads, out, held, sems = rest[:8], rest[8], rest[9], rest[10]
    loads = [pltpu.make_async_copy(grads[k], held.at[k], sems.at[k]) for k in range(8)]
    for c in loads:
        c.start()
    turned = acts[...].T
    for k in range(8):
        loads[k].wait()
        out[k] = (dot(turned, held[k]) + error[k].astype(F32)).astype(BF16)


def fed_of(acts, error, grads):
    return call(
        fed_body,
        on_chip((8, ROWS, COLS), BF16),
        6 * 10**9,
        16,
        in_specs=[VMEM, VMEM] + [HBM] * 8,
        out_specs=VMEM,
        scratch_shapes=[pltpu.VMEM((8, TOK, COLS), BF16), pltpu.SemaphoreType.DMA((8,))],
    )(acts, error, *grads)


def block_outputs(fed, basis, blocks, first, error_new, sketch_t, held, sems):
    stores = []
    scaled = (basis[...].astype(F32) * (1 / WORKERS)).astype(BF16)
    for i, tiles in enumerate(blocks):
        k = first + i
        where = block_at(k % 4, k >= 4)
        rows = [jnp.concatenate([tiles[4 * j + r] for j in range(6)], axis=1) for r in range(4)]
        block = jnp.concatenate(rows, axis=0)
        held[i] = (fed[k].astype(F32) - dot(scaled, block)).astype(BF16)
        store = pltpu.make_async_copy(held.at[i], error_new.at[0, :, columns(where)], sems.at[i])
        store.start()
        stores.append(store)
        sketch_t[:, columns(where)] = block
    return stores


def near_outputs_body(fed, basis, b0, b1, b2, b3, error_new, sketch_t, held, sems):
    stores = block_outputs(fed, basis, (b0, b1, b2, b3), 0, error_new, sketch_t, held, sems)
    for store in stores:
        store.wait()


OUTPUT_SCRATCH = [pltpu.VMEM((4, ROWS, COLS), BF16), pltpu.SemaphoreType.DMA((4,))]


def near_outputs(fed, basis, blocks):
    return call(
        near_outputs_body,
        (sds((1, ROWS, D), BF16), on_chip((RANK, D), BF16)),
        10**9,
        12,
        in_specs=[VMEM] * 6,
        out_specs=(HBM, VMEM),
        scratch_shapes=OUTPUT_SCRATCH,
    )(fed, basis, *blocks)


def far_outputs_body(
    fed, basis, b0, b1, b2, b3, momentum_t, _, near_t, error_new, momentum_new_t, sketch_t, held, sems
):
    for k in range(4):
        place = columns(block_at(k, False))
        sketch_t[:, place] = near_t[:, place]
    stores = block_outputs(fed, basis, (b0, b1, b2, b3), 4, error_new, sketch_t, held, sems)
    w = lax.axis_index(DP)
    quarter = lax.rem(w, 4)
    own = sketch_t[:, columns(w // 4)]
    part = own[:, 0:192]
    for i in (1, 2, 3):
        part = jnp.where(quarter == i, own[:, 192 * i : 192 * (i + 1)], part)
    part = part.astype(F32).T.astype(BF16)
    momentum_new_t[...] = BETA * momentum_t[...] + dot(part, basis[...], NT)
    for store in stores:
        store.wait()


def far_outputs(fed, basis, blocks, momentum_t, error_new, near_t):
    return call(
        far_outputs_body,
        (sds((1, ROWS, D), BF16), sds((192, ROWS), F32), sds((RANK, D), BF16)),
        10**9,
        12,
        in_specs=[VMEM] * 7 + [HBM, VMEM],
        out_specs=(HBM, VMEM, VMEM),
        scratch_shapes=OUTPUT_SCRATCH,
        input_output_aliases={7: 0},
    )(fed, basis, *blocks, momentum_t, error_new, near_t)


def along_y(x, k):
    return lax.ppermute(x, YY, [(i, (i + k) % 4) for i in range(4)])


def other_core(x):
    return lax.ppermute(x, CC, [(0, 1), (1, 0)])


def to_workers(x):
    return lax.all_to_all(x, DP, split_axis=0, concat_axis=0, tiled=True)


def after(x, *others):
    return lax.optimization_barrier((x, *others))[0]


def step(activations, out_grads, error, sketch, momentum):
    own_error = error[0]
    sketch_t = sketch.T

    mine = grads_sketch(out_grads, sketch_t)
    pair, rounded = pair_sum(mine, other_core(mine))
    others = []
    for k in (1, 2, 3):
        others.append(along_y(rounded, k))
    from_error, held_error = error_sketch(own_error, sketch_t)
    tiles = left_term(pair, others, activations, from_error)

    held = after(out_grads, *others)
    gathered = []
    for k in (1, 2, 3):
        gathered.append(along_y(held, -k % 4))

    arrived = to_workers(tiles)
    copies = sum_and_copy(arrived, F32)
    tiles = to_workers(copies)

    left, left_terms, small = left_products(tiles, activations)
    small = small + other_core(small)
    small_parts = [along_y(small, k) for k in (1, 2, 3)]
    send = right_far(left_terms, held_error)
    got = other_core(send)
    q = right_near(left_terms, held_error, got)
    terms = lax.all_to_all(q, YY, split_axis=0, concat_axis=0, tiled=True)
    inverse, basis, acts_left = factor(small, small_parts, left)
    pieces = right_term(inverse, acts_left, out_grads, terms)

    near_g = (out_grads, *gathered)
    far_g = []
    for k in range(4):
        far_g.append(other_core(after(near_g[k], pieces)))
    arrived = to_workers(pieces)
    copies = sum_and_copy(arrived, BF16)
    fed = fed_of(activations, held_error, (*near_g, *far_g))
    block = to_workers(copies)[:24]
    n3, n2, n1 = along_y(block, 1), along_y(block, 2), along_y(block, -1)
    near_n = (block, n1, n2, n3)
    far_n = []
    for k in range(4):
        far_n.append(other_core(near_n[k]))
    error_new, near_t = near_outputs(fed, basis, near_n)
    error_new, momentum_t, sketch_t = far_outputs(
        fed, basis, far_n, momentum.T, error_new, near_t
    )
    return error_new, momentum_t.T, sketch_t.T


def solution(mesh):
    split = Mesh(mesh.devices.reshape(8, 4, 4, 2), (*DP, YY, CC))
    mp = (YY, CC)
    return jax.shard_map(
        step,
        mesh=split,
        in_specs=(P(DP, mp), P(DP, mp), P(DP, mp, None), P(), P(mp, DP)),
        out_specs=(P(DP, mp, None), P(mp, DP), P()),
        check_vma=False,
    )
```

```python
import jax
import jax.numpy as jnp
from jax import lax
from jax.experimental import pallas as pl
from jax.experimental.pallas import tpu as pltpu
from jax.sharding import Mesh
from jax.sharding import PartitionSpec as P


DP = ("dp_0", "dp_1")
YY = "mp_0"
CC = "mp_1"
F32 = jnp.float32
BF16 = jnp.bfloat16
HIGHEST = lax.Precision.HIGHEST
D, RANK, ROWS, TOK, COLS, WORKERS = 6144, 64, 384, 512, 768, 32
INTERPRET = False
BETA = 0.9

NN = (((1,), (0,)), ((), ()))
NT = (((1,), (1,)), ((), ()))


def dot(a, b, dims=NN, precision=None):
    return lax.dot_general(a, b, dims, precision=precision, preferred_element_type=F32)


def two_terms(x):
    high = x.astype(BF16)
    low = (x - high.astype(F32)).astype(BF16)
    return jnp.concatenate([high, low], axis=0)


def halves_added(x):
    return x[: x.shape[0] // 2] + x[x.shape[0] // 2 :]


def call(body, out_shape, flops, mib=8, **kw):
    return pl.pallas_call(
        body,
        out_shape=out_shape,
        interpret=INTERPRET,
        compiler_params=pltpu.CompilerParams(vmem_limit_bytes=mib << 20),
        cost_estimate=pl.CostEstimate(flops=flops, bytes_accessed=1 << 20, transcendentals=0),
        **kw,
    )


def sds(shape, dtype):
    return jax.ShapeDtypeStruct(shape, dtype)


def on_chip(shape, dtype):
    return pltpu.VMEM(shape, dtype)


VMEM = pl.BlockSpec(memory_space=pltpu.VMEM)
HBM = pl.BlockSpec(memory_space=pltpu.HBM)


def block_at(ahead, other):
    y, c = lax.axis_index(YY), lax.axis_index(CC)
    return 2 * lax.rem(y + ahead, 4) + (1 - c if other else c)


def columns(block):
    return pl.ds(pl.multiple_of(block * COLS, COLS), COLS)


def grads_sketch_body(grads, sketch_t, out, held_s, held_g, sems):
    cut = pltpu.make_async_copy(
        sketch_t.at[:, columns(block_at(0, False))], held_s, sems.at[4]
    )
    cut.start()
    part = TOK // 4
    loads = [
        pltpu.make_async_copy(grads.at[pl.ds(part * i, part)], held_g.at[i], sems.at[i])
        for i in range(4)
    ]
    for c in loads:
        c.start()
    cut.wait()
    for i in range(4):
        loads[i].wait()
        out[:, part * i : part * (i + 1)] = dot(held_s[...], held_g[i], NT)


def grads_sketch(grads, sketch_t):
    return call(
        grads_sketch_body,
        on_chip((RANK, TOK), F32),
        10**8,
        in_specs=[HBM, HBM],
        out_specs=VMEM,
        scratch_shapes=[
            pltpu.VMEM((RANK, COLS), BF16),
            pltpu.VMEM((4, TOK // 4, COLS), BF16),
            pltpu.SemaphoreType.DMA((5,)),
        ],
    )(grads, sketch_t)


def pair_body(a, b, out, rounded):
    total = a[...] + b[...]
    out[...] = total
    rounded[...] = total.astype(BF16)


def pair_sum(a, b):
    return call(pair_body, (on_chip(a.shape, F32), on_chip(a.shape, BF16)), 10**7)(a, b)


def error_sketch_body(error, sketch_t, out, held, turned, sems):
    places = [columns(block_at(k % 4, k >= 4)) for k in range(8)]
    load = pltpu.make_async_copy(sketch_t, turned, sems.at[8])
    load.start()
    copies = [
        pltpu.make_async_copy(error.at[:, places[k]], held.at[k], sems.at[k]) for k in range(8)
    ]
    for c in copies:
        c.start()
    load.wait()
    acc = jnp.zeros((RANK, ROWS), F32)
    for k in range(8):
        copies[k].wait()
        acc = acc + dot(turned[:, places[k]], held[k], NT)
    out[...] = acc


def error_sketch(error, sketch_t):
    return call(
        error_sketch_body,
        on_chip((RANK, ROWS), F32),
        3 * 10**9,
        12,
        in_specs=[HBM, HBM],
        out_specs=VMEM,
        scratch_shapes=[
            pltpu.VMEM((8, ROWS, COLS), BF16),
            pltpu.VMEM((RANK, D), BF16),
            pltpu.SemaphoreType.DMA((9,)),
        ],
    )(error, sketch_t)


def left_term_body(own, one, two, three, acts, from_error, out):
    total = own[...] + one[...].astype(F32) + two[...].astype(F32) + three[...].astype(F32)
    left = halves_added(dot(two_terms(total), acts[...])) + from_error[...]
    for r in range(8):
        for j in range(3):
            out[4 * r + j] = left[8 * r : 8 * r + 8, 128 * j : 128 * j + 128]
        out[4 * r + 3] = jnp.zeros((8, 128), F32)


def left_term(own, parts, acts, from_error):
    return call(left_term_body, on_chip((WORKERS, 8, 128), F32), 10**8)(
        own, *parts, acts, from_error
    )


def sum_and_copy_body(arrived, out):
    total = jnp.sum(arrived[...].astype(F32), axis=0).astype(out.dtype)
    out[...] = jnp.broadcast_to(total[None], out.shape)


def sum_and_copy(arrived, dtype):
    return call(sum_and_copy_body, on_chip(arrived.shape, dtype), 10**7)(arrived)


def left_products_body(tiles, acts, left_out, left_terms, small):
    rows = [jnp.concatenate([tiles[4 * r + j] for j in range(3)], axis=1) for r in range(8)]
    left = jnp.concatenate(rows, axis=0)
    left_out[...] = left
    terms = two_terms(left)
    left_terms[...] = terms
    small[:, :TOK] = halves_added(dot(terms, acts[...], NT))
    gram = dot(left, left, NT, HIGHEST)
    small[:, TOK:] = jnp.concatenate([gram, jnp.zeros_like(gram)], axis=1)


def left_products(tiles, acts):
    return call(
        left_products_body,
        (
            on_chip((RANK, ROWS), F32),
            on_chip((2 * RANK, ROWS), BF16),
            on_chip((RANK, TOK + 128), F32),
        ),
        10**8,
    )(tiles, acts)


def right_blocks_body(left_terms, error, far, near, held, sems):
    y = lax.axis_index(YY)
    order = [(k, True) for k in range(4)] + [(k, False) for k in range(4)]
    copies = [
        pltpu.make_async_copy(error.at[:, columns(block_at(*o))], held.at[i], sems.at[i])
        for i, o in enumerate(order)
    ]
    for c in copies:
        c.start()
    for i, (k, other) in enumerate(order):
        copies[i].wait()
        out = far if other else near
        out[lax.rem(y + k, 4)] = halves_added(dot(left_terms[...], held[i]))


def right_blocks(left_terms, error):
    return call(
        right_blocks_body,
        (on_chip((4, RANK, COLS), F32), on_chip((4, RANK, COLS), F32)),
        10**10,
        12,
        in_specs=[VMEM, HBM],
        out_specs=(VMEM, VMEM),
        scratch_shapes=[pltpu.VMEM((8, ROWS, COLS), BF16), pltpu.SemaphoreType.DMA((8,))],
    )(left_terms, error)


def add_body(a, b, out):
    out[...] = a[...] + b[...]


def add(a, b):
    return call(add_body, on_chip(a.shape, F32), 10**7)(a, b)


def factor_body(own, one, two, three, left, inverse_out, basis_out, acts_left):
    small = own[...] + one[...] + two[...] + three[...]
    acts_left[...] = two_terms(small[:, :TOK])
    lanes = lax.broadcasted_iota(jnp.int32, (RANK, RANK), 1)
    subs = lax.broadcasted_iota(jnp.int32, (RANK, RANK), 0)
    eye = jnp.where(lanes == subs, 1.0, 0.0).astype(F32)
    work = jnp.concatenate([small[:, TOK : TOK + RANK], eye], axis=1)
    rows = lax.broadcasted_iota(jnp.int32, (RANK, 2 * RANK), 0)
    for j in range(RANK - 1):
        row = work[j : j + 1, :]
        ratio = work[:, j : j + 1] / work[j : j + 1, j : j + 1]
        work = work - jnp.where(rows > j, ratio * row, 0.0)
    pivots = jnp.sum(jnp.where(lanes == subs, work[:, :RANK], 0.0), axis=1, keepdims=True)
    inverse = work[:, RANK:] / jnp.sqrt(pivots)
    inverse_out[...] = inverse
    basis_out[...] = dot(inverse, left[...], NN, HIGHEST).T.astype(BF16)


def factor(own, parts, left):
    return call(
        factor_body,
        (on_chip((RANK, RANK), F32), on_chip((ROWS, RANK), BF16), on_chip((2 * RANK, TOK), BF16)),
        6 * 10**9,
    )(own, *parts, left)


def right_term_body(inverse, acts_left, grads, terms, out):
    total = terms[0] + terms[1] + terms[2] + terms[3]
    total = total + halves_added(dot(acts_left[...], grads[...]))
    right = dot(inverse[...], total, NN, HIGHEST)
    for j in range(6):
        for r in range(4):
            out[4 * j + r] = right[16 * r : 16 * r + 16, 128 * j : 128 * j + 128].astype(out.dtype)
    out[24:] = jnp.zeros((8, 16, 128), out.dtype)


def right_term(inverse, acts_left, grads, terms):
    return call(right_term_body, on_chip((WORKERS, 16, 128), BF16), 10**8)(
        inverse, acts_left, grads, terms
    )


def fed_body(acts, error, *rest):
    grads, out, held, held_e, held_o, sems = rest[:8], rest[8], *rest[9:]
    errors = [
        pltpu.make_async_copy(
            error.at[:, columns(block_at(k % 4, k >= 4))], held_e.at[k], sems.at[k]
        )
        for k in range(8)
    ]
    loads = [pltpu.make_async_copy(grads[k], held.at[k], sems.at[8 + k]) for k in range(8)]
    for k in range(8):
        loads[k].start()
        errors[k].start()
    turned = acts[...].T
    stores = []
    for k in range(8):
        loads[k].wait()
        errors[k].wait()
        held_o[k] = (dot(turned, held[k]) + held_e[k].astype(F32)).astype(BF16)
        store = pltpu.make_async_copy(held_o.at[k], out.at[k], sems.at[16 + k])
        store.start()
        stores.append(store)
    for store in stores:
        store.wait()


def fed_of(acts, error, grads):
    return call(
        fed_body,
        pltpu.HBM((8, ROWS, COLS), BF16),
        6 * 10**9,
        24,
        in_specs=[VMEM, HBM] + [HBM] * 8,
        out_specs=HBM,
        scratch_shapes=[
            pltpu.VMEM((8, TOK, COLS), BF16),
            pltpu.VMEM((8, ROWS, COLS), BF16),
            pltpu.VMEM((8, ROWS, COLS), BF16),
            pltpu.SemaphoreType.DMA((24,)),
        ],
    )(acts, error, *map(in_hbm, grads))


def block_outputs(fed, first, basis, blocks, error_new, sketch_t, held, sems):
    stores = []
    scaled = (basis[...].astype(F32) * (1 / WORKERS)).astype(BF16)
    for i, tiles in enumerate(blocks):
        k = first + i
        where = block_at(k % 4, k >= 4)
        rows = [jnp.concatenate([tiles[4 * j + r] for j in range(6)], axis=1) for r in range(4)]
        block = jnp.concatenate(rows, axis=0)
        held[i] = (fed[i].astype(F32) - dot(scaled, block)).astype(BF16)
        store = pltpu.make_async_copy(held.at[i], error_new.at[0, :, columns(where)], sems.at[i])
        store.start()
        stores.append(store)
        sketch_t[:, columns(where)] = block
    return stores


def near_outputs_body(
    fed, basis, b0, b1, b2, b3, error_new, sketch_t, fed_far, held_f, held, sems, load_sems
):
    loads = [
        pltpu.make_async_copy(
            fed.at[k], held_f.at[k] if k < 4 else fed_far.at[k - 4], load_sems.at[k]
        )
        for k in range(8)
    ]
    for c in loads:
        c.start()
    for c in loads[:4]:
        c.wait()
    stores = block_outputs(held_f, 0, basis, (b0, b1, b2, b3), error_new, sketch_t, held, sems)
    for c in loads[4:] + stores:
        c.wait()


def near_outputs(fed, basis, blocks):
    return call(
        near_outputs_body,
        (sds((1, ROWS, D), BF16), on_chip((RANK, D), BF16), on_chip((4, ROWS, COLS), BF16)),
        10**9,
        12,
        in_specs=[HBM] + [VMEM] * 5,
        out_specs=(HBM, VMEM, VMEM),
        scratch_shapes=[
            pltpu.VMEM((4, ROWS, COLS), BF16),
            pltpu.VMEM((4, ROWS, COLS), BF16),
            pltpu.SemaphoreType.DMA((4,)),
            pltpu.SemaphoreType.DMA((8,)),
        ],
    )(fed, basis, *blocks)


def far_outputs_body(
    fed, basis, b0, b1, b2, b3, momentum_t, _, near_t, error_new, momentum_new_t, sketch_t, held, sems
):
    for k in range(4):
        place = columns(block_at(k, False))
        sketch_t[:, place] = near_t[:, place]
    stores = block_outputs(fed, 4, basis, (b0, b1, b2, b3), error_new, sketch_t, held, sems)
    w = lax.axis_index(DP)
    quarter = lax.rem(w, 4)
    own = sketch_t[:, columns(w // 4)]
    part = own[:, 0:192]
    for i in (1, 2, 3):
        part = jnp.where(quarter == i, own[:, 192 * i : 192 * (i + 1)], part)
    part = part.astype(F32).T.astype(BF16)
    momentum_new_t[...] = BETA * momentum_t[...] + dot(part, basis[...], NT)
    for store in stores:
        store.wait()


def far_outputs(fed_far, basis, blocks, momentum_t, error_new, near_t):
    return call(
        far_outputs_body,
        (sds((1, ROWS, D), BF16), sds((192, ROWS), F32), sds((RANK, D), BF16)),
        10**9,
        12,
        in_specs=[VMEM] * 7 + [HBM, VMEM],
        out_specs=(HBM, VMEM, VMEM),
        scratch_shapes=[pltpu.VMEM((4, ROWS, COLS), BF16), pltpu.SemaphoreType.DMA((4,))],
        input_output_aliases={7: 0},
    )(fed_far, basis, *blocks, momentum_t, error_new, near_t)


def along_y(x, k):
    return lax.ppermute(x, YY, [(i, (i + k) % 4) for i in range(4)])


def other_core(x):
    return lax.ppermute(x, CC, [(0, 1), (1, 0)])


def to_workers(x):
    return lax.all_to_all(x, DP, split_axis=0, concat_axis=0, tiled=True)


def in_hbm(x):
    return pltpu.with_memory_space_constraint(x, pltpu.HBM)


def after(x, *others):
    return lax.optimization_barrier((x, *others))[0]


def step(activations, out_grads, error, sketch, momentum):
    own_error = in_hbm(error[0])
    sketch_t = in_hbm(sketch.T)
    own_grads, out_grads = out_grads, in_hbm(out_grads)

    mine = grads_sketch(out_grads, sketch_t)
    pair, rounded = pair_sum(mine, other_core(mine))
    others = []
    for k in (1, 2, 3):
        others.append(along_y(rounded, k))
    from_error = error_sketch(own_error, sketch_t)
    tiles = left_term(pair, others, activations, from_error)

    held = after(out_grads, *others)
    gathered = []
    for k in (1, 2, 3):
        gathered.append(along_y(held, -k % 4))

    arrived = to_workers(tiles)
    copies = sum_and_copy(arrived, F32)
    tiles = to_workers(copies)

    left, left_terms, small = left_products(tiles, activations)
    other_small = other_core(small)
    far, near = right_blocks(left_terms, own_error)
    got = other_core(far)
    small_parts = []
    small = add(small, other_small)
    for k in (1, 2, 3):
        small_parts.append(along_y(small, k))
    q = add(near, got)
    terms = lax.all_to_all(q, YY, split_axis=0, concat_axis=0, tiled=True)
    inverse, basis, acts_left = factor(small, small_parts, left)
    pieces = right_term(inverse, acts_left, own_grads, terms)

    near_g = (out_grads, *gathered)
    far_g = []
    for k in range(4):
        far_g.append(other_core(after(near_g[k], pieces)))
    arrived = to_workers(pieces)
    copies = sum_and_copy(arrived, BF16)
    fed = fed_of(activations, own_error, (*near_g, *far_g))
    block = to_workers(copies)[:24]
    n3, n2, n1 = along_y(block, 1), along_y(block, 2), along_y(block, -1)
    near_n = (block, n1, n2, n3)
    far_n = []
    for k in range(4):
        far_n.append(other_core(near_n[k]))
    error_new, near_t, fed_far = near_outputs(in_hbm(fed), basis, near_n)
    error_new, momentum_t, sketch_t = far_outputs(
        fed_far, basis, far_n, momentum.T, error_new, near_t
    )
    return error_new, momentum_t.T, sketch_t.T


def solution(mesh):
    split = Mesh(mesh.devices.reshape(8, 4, 4, 2), (*DP, YY, CC))
    mp = (YY, CC)
    return jax.shard_map(
        step,
        mesh=split,
        in_specs=(P(DP, mp), P(DP, mp), P(DP, mp, None), P(), P(mp, DP)),
        out_specs=(P(DP, mp, None), P(mp, DP), P()),
        check_vma=False,
    )
```

```python
import jax
import jax.numpy as jnp
from jax import lax
from jax.experimental import pallas as pl
from jax.experimental.pallas import tpu as pltpu
from jax.sharding import Mesh
from jax.sharding import PartitionSpec as P


DP = ("dp_0", "dp_1")
YY = "mp_0"
CC = "mp_1"
F32 = jnp.float32
BF16 = jnp.bfloat16
HIGHEST = lax.Precision.HIGHEST
D, RANK, ROWS, TOK, COLS, WORKERS = 6144, 64, 384, 512, 768, 32
INTERPRET = False
BETA = 0.9

NN = (((1,), (0,)), ((), ()))
NT = (((1,), (1,)), ((), ()))


def dot(a, b, dims=NN, precision=None):
    return lax.dot_general(a, b, dims, precision=precision, preferred_element_type=F32)


def two_terms(x):
    high = x.astype(BF16)
    low = (x - high.astype(F32)).astype(BF16)
    return jnp.concatenate([high, low], axis=0)


def halves_added(x):
    return x[: x.shape[0] // 2] + x[x.shape[0] // 2 :]


def call(body, out_shape, flops, mib=8, **kw):
    return pl.pallas_call(
        body,
        out_shape=out_shape,
        interpret=INTERPRET,
        compiler_params=pltpu.CompilerParams(vmem_limit_bytes=mib << 20),
        cost_estimate=pl.CostEstimate(flops=flops, bytes_accessed=1 << 20, transcendentals=0),
        **kw,
    )


def sds(shape, dtype):
    return jax.ShapeDtypeStruct(shape, dtype)


def on_chip(shape, dtype):
    return pltpu.VMEM(shape, dtype)


VMEM = pl.BlockSpec(memory_space=pltpu.VMEM)
HBM = pl.BlockSpec(memory_space=pltpu.HBM)


def block_at(ahead, other):
    y, c = lax.axis_index(YY), lax.axis_index(CC)
    return 2 * lax.rem(y + ahead, 4) + (1 - c if other else c)


def columns(block):
    return pl.ds(pl.multiple_of(block * COLS, COLS), COLS)


def grads_sketch_body(grads, sketch_t, out, held_s, held_g, sems):
    cut = pltpu.make_async_copy(
        sketch_t.at[:, columns(block_at(0, False))], held_s, sems.at[4]
    )
    cut.start()
    part = TOK // 4
    loads = [
        pltpu.make_async_copy(grads.at[pl.ds(part * i, part)], held_g.at[i], sems.at[i])
        for i in range(4)
    ]
    for c in loads:
        c.start()
    cut.wait()
    for i in range(4):
        loads[i].wait()
        out[:, part * i : part * (i + 1)] = dot(held_s[...], held_g[i], NT)


def grads_sketch(grads, sketch_t):
    return call(
        grads_sketch_body,
        on_chip((RANK, TOK), F32),
        10**8,
        in_specs=[HBM, HBM],
        out_specs=VMEM,
        scratch_shapes=[
            pltpu.VMEM((RANK, COLS), BF16),
            pltpu.VMEM((4, TOK // 4, COLS), BF16),
            pltpu.SemaphoreType.DMA((5,)),
        ],
    )(grads, sketch_t)


def pair_body(a, b, out, rounded):
    total = a[...] + b[...]
    out[...] = total
    rounded[...] = total.astype(BF16)


def pair_sum(a, b):
    return call(pair_body, (on_chip(a.shape, F32), on_chip(a.shape, BF16)), 10**7)(a, b)


def error_sketch_body(error, sketch_t, out, held, turned, sems):
    places = [columns(block_at(k % 4, k >= 4)) for k in range(8)]
    load = pltpu.make_async_copy(sketch_t, turned, sems.at[8])
    load.start()
    copies = [
        pltpu.make_async_copy(error.at[:, places[k]], held.at[k], sems.at[k]) for k in range(8)
    ]
    for c in copies:
        c.start()
    load.wait()
    acc = jnp.zeros((RANK, ROWS), F32)
    for k in range(8):
        copies[k].wait()
        acc = acc + dot(turned[:, places[k]], held[k], NT)
    out[...] = acc


def error_sketch(error, sketch_t):
    return call(
        error_sketch_body,
        on_chip((RANK, ROWS), F32),
        3 * 10**9,
        12,
        in_specs=[HBM, HBM],
        out_specs=VMEM,
        scratch_shapes=[
            pltpu.VMEM((8, ROWS, COLS), BF16),
            pltpu.VMEM((RANK, D), BF16),
            pltpu.SemaphoreType.DMA((9,)),
        ],
    )(error, sketch_t)


def left_term_body(own, one, two, three, acts, from_error, out):
    total = own[...] + one[...].astype(F32) + two[...].astype(F32) + three[...].astype(F32)
    left = halves_added(dot(two_terms(total), acts[...])) + from_error[...]
    for r in range(8):
        for j in range(3):
            out[4 * r + j] = left[8 * r : 8 * r + 8, 128 * j : 128 * j + 128]
        out[4 * r + 3] = jnp.zeros((8, 128), F32)


def left_term(own, parts, acts, from_error):
    return call(left_term_body, on_chip((WORKERS, 8, 128), F32), 10**8)(
        own, *parts, acts, from_error
    )


def sum_and_copy_body(arrived, out):
    total = jnp.sum(arrived[...].astype(F32), axis=0).astype(out.dtype)
    out[...] = jnp.broadcast_to(total[None], out.shape)


def sum_and_copy(arrived, dtype):
    return call(sum_and_copy_body, on_chip(arrived.shape, dtype), 10**7)(arrived)


def left_products_body(tiles, acts, left_out, left_terms, small):
    rows = [jnp.concatenate([tiles[4 * r + j] for j in range(3)], axis=1) for r in range(8)]
    left = jnp.concatenate(rows, axis=0)
    left_out[...] = left
    terms = two_terms(left)
    left_terms[...] = terms
    small[:, :TOK] = halves_added(dot(terms, acts[...], NT))
    gram = dot(left, left, NT, HIGHEST)
    small[:, TOK:] = jnp.concatenate([gram, jnp.zeros_like(gram)], axis=1)


def left_products(tiles, acts):
    return call(
        left_products_body,
        (
            on_chip((RANK, ROWS), F32),
            on_chip((2 * RANK, ROWS), BF16),
            on_chip((RANK, TOK + 128), F32),
        ),
        10**8,
    )(tiles, acts)


def right_blocks_body(left_terms, error, far, near, held, sems):
    y = lax.axis_index(YY)
    order = [(k, True) for k in range(4)] + [(k, False) for k in range(4)]
    copies = [
        pltpu.make_async_copy(error.at[:, columns(block_at(*o))], held.at[i], sems.at[i])
        for i, o in enumerate(order)
    ]
    for c in copies:
        c.start()
    for i, (k, other) in enumerate(order):
        copies[i].wait()
        out = far if other else near
        out[lax.rem(y + k, 4)] = halves_added(dot(left_terms[...], held[i]))


def right_blocks(left_terms, error):
    return call(
        right_blocks_body,
        (on_chip((4, RANK, COLS), F32), on_chip((4, RANK, COLS), F32)),
        10**10,
        12,
        in_specs=[VMEM, HBM],
        out_specs=(VMEM, VMEM),
        scratch_shapes=[pltpu.VMEM((8, ROWS, COLS), BF16), pltpu.SemaphoreType.DMA((8,))],
    )(left_terms, error)


def add_body(a, b, out):
    out[...] = a[...] + b[...]


def add(a, b):
    return call(add_body, on_chip(a.shape, F32), 10**7)(a, b)


def factor_body(own, one, two, three, left, inverse_out, basis_out, acts_left):
    small = own[...] + one[...] + two[...] + three[...]
    acts_left[...] = two_terms(small[:, :TOK])
    lanes = lax.broadcasted_iota(jnp.int32, (RANK, RANK), 1)
    subs = lax.broadcasted_iota(jnp.int32, (RANK, RANK), 0)
    eye = jnp.where(lanes == subs, 1.0, 0.0).astype(F32)
    work = jnp.concatenate([small[:, TOK : TOK + RANK], eye], axis=1)
    rows = lax.broadcasted_iota(jnp.int32, (RANK, 2 * RANK), 0)
    for j in range(RANK - 1):
        row = work[j : j + 1, :]
        ratio = work[:, j : j + 1] / work[j : j + 1, j : j + 1]
        work = work - jnp.where(rows > j, ratio * row, 0.0)
    pivots = jnp.sum(jnp.where(lanes == subs, work[:, :RANK], 0.0), axis=1, keepdims=True)
    inverse = work[:, RANK:] / jnp.sqrt(pivots)
    inverse_out[...] = inverse
    basis_out[...] = dot(inverse, left[...], NN, HIGHEST).T.astype(BF16)


def factor(own, parts, left):
    return call(
        factor_body,
        (on_chip((RANK, RANK), F32), on_chip((ROWS, RANK), BF16), on_chip((2 * RANK, TOK), BF16)),
        6 * 10**9,
    )(own, *parts, left)


def right_term_body(inverse, acts_left, grads, terms, out):
    total = terms[0] + terms[1] + terms[2] + terms[3]
    total = total + halves_added(dot(acts_left[...], grads[...]))
    right = dot(inverse[...], total, NN, HIGHEST)
    for j in range(6):
        for r in range(4):
            out[4 * j + r] = right[16 * r : 16 * r + 16, 128 * j : 128 * j + 128].astype(out.dtype)
    out[24:] = jnp.zeros((8, 16, 128), out.dtype)


def right_term(inverse, acts_left, grads, terms):
    return call(right_term_body, on_chip((WORKERS, 16, 128), BF16), 10**8)(
        inverse, acts_left, grads, terms
    )


def copies_of_grads(pieces, place, sems):
    own, up, half_a, half_b, down = pieces
    h = TOK // 2
    return [
        [pltpu.make_async_copy(own, place.at[0], sems.at[0])],
        [pltpu.make_async_copy(up, place.at[1], sems.at[1])],
        [
            pltpu.make_async_copy(half_a, place.at[2, pl.ds(0, h)], sems.at[2]),
            pltpu.make_async_copy(half_b, place.at[2, pl.ds(h, h)], sems.at[3]),
        ],
        [pltpu.make_async_copy(down, place.at[3], sems.at[4])],
    ]


def fed_body(acts, error, *rest):
    grads, out, held, held_e, held_o, sems, near_sems, far_sems = rest[:10], *rest[10:]
    errors = [
        pltpu.make_async_copy(
            error.at[:, columns(block_at(k % 4, k >= 4))], held_e.at[k], sems.at[k]
        )
        for k in range(8)
    ]
    loads = copies_of_grads(grads[:5], held.at[pl.ds(0, 4)], near_sems)
    loads += copies_of_grads(grads[5:], held.at[pl.ds(4, 4)], far_sems)
    for k in range(8):
        for c in loads[k]:
            c.start()
        errors[k].start()
    turned = acts[...].T
    stores = []
    for k in range(8):
        for c in loads[k]:
            c.wait()
        errors[k].wait()
        held_o[k] = (dot(turned, held[k]) + held_e[k].astype(F32)).astype(BF16)
        store = pltpu.make_async_copy(held_o.at[k], out.at[k], sems.at[8 + k])
        store.start()
        stores.append(store)
    for store in stores:
        store.wait()


def fed_of(acts, error, grads):
    return call(
        fed_body,
        pltpu.HBM((8, ROWS, COLS), BF16),
        6 * 10**9,
        24,
        in_specs=[VMEM, HBM] + [HBM] * 10,
        out_specs=HBM,
        scratch_shapes=[
            pltpu.VMEM((8, TOK, COLS), BF16),
            pltpu.VMEM((8, ROWS, COLS), BF16),
            pltpu.VMEM((8, ROWS, COLS), BF16),
            pltpu.SemaphoreType.DMA((16,)),
            pltpu.SemaphoreType.DMA((5,)),
            pltpu.SemaphoreType.DMA((5,)),
        ],
    )(acts, error, *map(in_hbm, grads))


def joined(tiles):
    rows = [jnp.concatenate([tiles[4 * j + r] for j in range(6)], axis=1) for r in range(4)]
    return jnp.concatenate(rows, axis=0)


def block_outputs(fed, first, basis, blocks, error_new, sketch_t, held, sems):
    stores = []
    scaled = (basis[...].astype(F32) * (1 / WORKERS)).astype(BF16)
    for i, tiles in enumerate(blocks):
        k = first + i
        where = block_at(k % 4, k >= 4)
        block = joined(tiles)
        held[i] = (fed[i].astype(F32) - dot(scaled, block)).astype(BF16)
        store = pltpu.make_async_copy(held.at[i], error_new.at[0, :, columns(where)], sems.at[i])
        store.start()
        stores.append(store)
        sketch_t[:, columns(where)] = block
    return stores


def own_outputs_body(
    fed, basis, b0, error_new, sketch_t, fed_near, fed_far, held_f, held, sems, load_sems
):
    places = [held_f.at[0]] + [fed_near.at[k] for k in range(3)] + [fed_far.at[k] for k in range(4)]
    loads = [
        pltpu.make_async_copy(fed.at[k], places[k], load_sems.at[k]) for k in range(8)
    ]
    for c in loads:
        c.start()
    loads[0].wait()
    stores = block_outputs(held_f, 0, basis, (b0,), error_new, sketch_t, held, sems)
    for c in loads[1:] + stores:
        c.wait()


def own_outputs(fed, basis, b0):
    return call(
        own_outputs_body,
        (
            sds((1, ROWS, D), BF16),
            on_chip((RANK, D), BF16),
            on_chip((3, ROWS, COLS), BF16),
            on_chip((4, ROWS, COLS), BF16),
        ),
        10**9,
        8,
        in_specs=[HBM, VMEM, VMEM],
        out_specs=(HBM, VMEM, VMEM, VMEM),
        scratch_shapes=[
            pltpu.VMEM((1, ROWS, COLS), BF16),
            pltpu.VMEM((1, ROWS, COLS), BF16),
            pltpu.SemaphoreType.DMA((1,)),
            pltpu.SemaphoreType.DMA((8,)),
        ],
    )(fed, basis, b0)


def near_outputs_body(fed, basis, b1, b2, b3, _, own_t, error_new, sketch_t, held, sems):
    place = columns(block_at(0, False))
    sketch_t[:, place] = own_t[:, place]
    stores = block_outputs(fed, 1, basis, (b1, b2, b3), error_new, sketch_t, held, sems)
    for c in stores:
        c.wait()


def near_outputs(fed_near, basis, blocks, error_new, own_t):
    return call(
        near_outputs_body,
        (sds((1, ROWS, D), BF16), on_chip((RANK, D), BF16)),
        10**9,
        8,
        in_specs=[VMEM] * 5 + [HBM, VMEM],
        out_specs=(HBM, VMEM),
        scratch_shapes=[pltpu.VMEM((3, ROWS, COLS), BF16), pltpu.SemaphoreType.DMA((3,))],
        input_output_aliases={5: 0},
    )(fed_near, basis, *blocks, error_new, own_t)


def far_outputs_body(
    fed, basis, b0, b1, b2, b3, momentum_t, _, near_t, error_new, momentum_new_t, sketch_t, held, sems
):
    for k in range(4):
        place = columns(block_at(k, False))
        sketch_t[:, place] = near_t[:, place]
    stores = block_outputs(fed, 4, basis, (b0, b1, b2, b3), error_new, sketch_t, held, sems)
    w = lax.axis_index(DP)
    quarter = lax.rem(w, 4)
    own = sketch_t[:, columns(w // 4)]
    part = own[:, 0:192]
    for i in (1, 2, 3):
        part = jnp.where(quarter == i, own[:, 192 * i : 192 * (i + 1)], part)
    part = part.astype(F32).T.astype(BF16)
    momentum_new_t[...] = BETA * momentum_t[...] + dot(part, basis[...], NT)
    for store in stores:
        store.wait()


def far_outputs(fed_far, basis, blocks, momentum_t, error_new, near_t):
    return call(
        far_outputs_body,
        (sds((1, ROWS, D), BF16), sds((192, ROWS), F32), sds((RANK, D), BF16)),
        10**9,
        12,
        in_specs=[VMEM] * 7 + [HBM, VMEM],
        out_specs=(HBM, VMEM, VMEM),
        scratch_shapes=[pltpu.VMEM((4, ROWS, COLS), BF16), pltpu.SemaphoreType.DMA((4,))],
        input_output_aliases={7: 0},
    )(fed_far, basis, *blocks, momentum_t, error_new, near_t)


def along_y(x, k):
    return lax.ppermute(x, YY, [(i, (i + k) % 4) for i in range(4)])


def other_core(x):
    return lax.ppermute(x, CC, [(0, 1), (1, 0)])


def to_workers(x):
    return lax.all_to_all(x, DP, split_axis=0, concat_axis=0, tiled=True)


def in_hbm(x):
    return pltpu.with_memory_space_constraint(x, pltpu.HBM)


def after(x, *others):
    return lax.optimization_barrier((x, *others))[0]


def step(activations, out_grads, error, sketch, momentum):
    own_error = in_hbm(error[0])
    sketch_t = in_hbm(sketch.T)
    own_grads, out_grads = out_grads, in_hbm(out_grads)

    mine = grads_sketch(out_grads, sketch_t)
    pair, rounded = pair_sum(mine, other_core(mine))
    others = []
    for k in (1, 2, 3):
        others.append(along_y(rounded, k))
    from_error = error_sketch(own_error, sketch_t)
    tiles = left_term(pair, others, activations, from_error)

    held = after(own_grads, *others)
    g1 = along_y(held, -1)
    g3 = along_y(held, 1)

    arrived = to_workers(tiles)
    copies = sum_and_copy(arrived, F32)
    tiles = to_workers(copies)

    left, left_terms, small = left_products(tiles, activations)
    other_small = other_core(small)
    far, near = right_blocks(left_terms, own_error)
    got = other_core(far)
    small_parts = []
    small = add(small, other_small)
    for k in (1, 2, 3):
        small_parts.append(along_y(small, k))
    q = add(near, got)
    terms = lax.all_to_all(q, YY, split_axis=0, concat_axis=0, tiled=True)
    inverse, basis, acts_left = factor(small, small_parts, left)
    pieces = right_term(inverse, acts_left, own_grads, terms)

    half = TOK // 2
    g2a = along_y(after(g1, pieces)[:half], -1)
    g2b = along_y(after(g3, pieces)[half:], 1)
    near_g = (own_grads, g1, g2a, g2b, g3)
    far_g = []
    for k in range(5):
        far_g.append(other_core(after(near_g[k], pieces)))
    arrived = to_workers(pieces)
    copies = sum_and_copy(arrived, BF16)
    fed = fed_of(activations, own_error, (*near_g, *far_g))
    block = to_workers(copies)[:24]
    spread = []
    for k in (1, 2, 3):
        spread.append(along_y(block, -k % 4))
    near_n = (block, *spread)
    far_n = []
    for k in range(4):
        far_n.append(other_core(near_n[k]))
    error_new, own_t, fed_near, fed_far = own_outputs(in_hbm(fed), basis, block)
    error_new, near_t = near_outputs(fed_near, basis, spread, error_new, own_t)
    error_new, momentum_t, sketch_t = far_outputs(
        fed_far, basis, far_n, momentum.T, error_new, near_t
    )
    return error_new, momentum_t.T, sketch_t.T


def solution(mesh):
    split = Mesh(mesh.devices.reshape(8, 4, 4, 2), (*DP, YY, CC))
    mp = (YY, CC)
    return jax.shard_map(
        step,
        mesh=split,
        in_specs=(P(DP, mp), P(DP, mp), P(DP, mp, None), P(), P(mp, DP)),
        out_specs=(P(DP, mp, None), P(mp, DP), P()),
        check_vma=False,
    )
```

```python
import jax
import jax.numpy as jnp
from jax import lax
from jax.experimental import pallas as pl
from jax.experimental.pallas import tpu as pltpu
from jax.sharding import Mesh
from jax.sharding import PartitionSpec as P


DP = ("dp_0", "dp_1")
YY = "mp_0"
CC = "mp_1"
F32 = jnp.float32
BF16 = jnp.bfloat16
HIGHEST = lax.Precision.HIGHEST
D, RANK, ROWS, TOK, COLS, WORKERS = 6144, 64, 384, 512, 768, 32
INTERPRET = False
BETA = 0.9

NN = (((1,), (0,)), ((), ()))
NT = (((1,), (1,)), ((), ()))


def dot(a, b, dims=NN, precision=None):
    return lax.dot_general(a, b, dims, precision=precision, preferred_element_type=F32)


def two_terms(x):
    high = x.astype(BF16)
    low = (x - high.astype(F32)).astype(BF16)
    return jnp.concatenate([high, low], axis=0)


def halves_added(x):
    return x[: x.shape[0] // 2] + x[x.shape[0] // 2 :]


def call(body, out_shape, flops, mib=8, **kw):
    return pl.pallas_call(
        body,
        out_shape=out_shape,
        interpret=INTERPRET,
        compiler_params=pltpu.CompilerParams(vmem_limit_bytes=mib << 20),
        cost_estimate=pl.CostEstimate(flops=flops, bytes_accessed=1 << 20, transcendentals=0),
        **kw,
    )


def sds(shape, dtype):
    return jax.ShapeDtypeStruct(shape, dtype)


def on_chip(shape, dtype):
    return pltpu.VMEM(shape, dtype)


VMEM = pl.BlockSpec(memory_space=pltpu.VMEM)
HBM = pl.BlockSpec(memory_space=pltpu.HBM)


def block_at(ahead, other):
    y, c = lax.axis_index(YY), lax.axis_index(CC)
    return 2 * lax.rem(y + ahead, 4) + (1 - c if other else c)


def columns(block):
    return pl.ds(pl.multiple_of(block * COLS, COLS), COLS)


def grads_sketch_body(grads, sketch_t, out, held_s, held_g, sems):
    cut = pltpu.make_async_copy(
        sketch_t.at[:, columns(block_at(0, False))], held_s, sems.at[4]
    )
    cut.start()
    part = TOK // 4
    loads = [
        pltpu.make_async_copy(grads.at[pl.ds(part * i, part)], held_g.at[i], sems.at[i])
        for i in range(4)
    ]
    for c in loads:
        c.start()
    cut.wait()
    for i in range(4):
        loads[i].wait()
        out[:, part * i : part * (i + 1)] = dot(held_s[...], held_g[i], NT)


def grads_sketch(grads, sketch_t):
    return call(
        grads_sketch_body,
        on_chip((RANK, TOK), F32),
        10**8,
        in_specs=[HBM, HBM],
        out_specs=VMEM,
        scratch_shapes=[
            pltpu.VMEM((RANK, COLS), BF16),
            pltpu.VMEM((4, TOK // 4, COLS), BF16),
            pltpu.SemaphoreType.DMA((5,)),
        ],
    )(grads, sketch_t)


def pair_body(a, b, out, rounded):
    total = a[...] + b[...]
    out[...] = total
    rounded[...] = total.astype(BF16)


def pair_sum(a, b):
    return call(pair_body, (on_chip(a.shape, F32), on_chip(a.shape, BF16)), 10**7)(a, b)


def error_sketch_body(error, sketch_t, out, held, turned, sems):
    places = [columns(block_at(k % 4, k >= 4)) for k in range(8)]
    load = pltpu.make_async_copy(sketch_t, turned, sems.at[8])
    load.start()
    copies = [
        pltpu.make_async_copy(error.at[:, places[k]], held.at[k], sems.at[k]) for k in range(8)
    ]
    for c in copies:
        c.start()
    load.wait()
    acc = jnp.zeros((RANK, ROWS), F32)
    for k in range(8):
        copies[k].wait()
        acc = acc + dot(turned[:, places[k]], held[k], NT)
    out[...] = acc


def error_sketch(error, sketch_t):
    return call(
        error_sketch_body,
        on_chip((RANK, ROWS), F32),
        3 * 10**9,
        12,
        in_specs=[HBM, HBM],
        out_specs=VMEM,
        scratch_shapes=[
            pltpu.VMEM((8, ROWS, COLS), BF16),
            pltpu.VMEM((RANK, D), BF16),
            pltpu.SemaphoreType.DMA((9,)),
        ],
    )(error, sketch_t)


def left_term_body(own, one, two, three, acts, from_error, out):
    total = own[...] + one[...].astype(F32) + two[...].astype(F32) + three[...].astype(F32)
    left = halves_added(dot(two_terms(total), acts[...])) + from_error[...]
    for r in range(8):
        for j in range(3):
            out[4 * r + j] = left[8 * r : 8 * r + 8, 128 * j : 128 * j + 128]
        out[4 * r + 3] = jnp.zeros((8, 128), F32)


def left_term(own, parts, acts, from_error):
    return call(left_term_body, on_chip((WORKERS, 8, 128), F32), 10**8)(
        own, *parts, acts, from_error
    )


def sum_and_copy_body(arrived, out):
    total = jnp.sum(arrived[...].astype(F32), axis=0).astype(out.dtype)
    out[...] = jnp.broadcast_to(total[None], out.shape)


def sum_and_copy(arrived, dtype):
    return call(sum_and_copy_body, on_chip(arrived.shape, dtype), 10**7)(arrived)


HALF = TOK // 2


def left_products_body(tiles, acts, left_out, left_terms, mine, theirs):
    rows = [jnp.concatenate([tiles[4 * r + j] for j in range(3)], axis=1) for r in range(8)]
    left = jnp.concatenate(rows, axis=0)
    left_out[...] = left
    terms = two_terms(left)
    left_terms[...] = terms
    acts_left = halves_added(dot(terms, acts[...], NT))
    gram = dot(left, left, NT, HIGHEST)
    gram = jnp.concatenate([gram, jnp.zeros_like(gram)], axis=1)
    first = lax.axis_index(CC) == 0
    low, high = acts_left[:, :HALF], acts_left[:, HALF:]
    mine[:, :HALF] = jnp.where(first, low, high)
    mine[:, HALF:] = gram
    theirs[:, :HALF] = jnp.where(first, high, low)
    theirs[:, HALF:] = gram


def left_products(tiles, acts):
    return call(
        left_products_body,
        (
            on_chip((RANK, ROWS), F32),
            on_chip((2 * RANK, ROWS), BF16),
            on_chip((RANK, HALF + 128), F32),
            on_chip((RANK, HALF + 128), F32),
        ),
        10**8,
    )(tiles, acts)


def small_sum_body(own, one, two, three, acts_left, gram):
    total = own[...] + one[...] + two[...] + three[...]
    acts_left[...] = total[:, :HALF]
    gram[...] = total[:, HALF:]


def small_sum(own, parts):
    return call(
        small_sum_body, (on_chip((RANK, HALF), F32), on_chip((RANK, 128), F32)), 10**7
    )(own, *parts)


def right_blocks_body(left_terms, error, far, near, held, sems):
    y = lax.axis_index(YY)
    order = [(k, True) for k in range(4)] + [(k, False) for k in range(4)]
    copies = [
        pltpu.make_async_copy(error.at[:, columns(block_at(*o))], held.at[i], sems.at[i])
        for i, o in enumerate(order)
    ]
    for c in copies:
        c.start()
    for i, (k, other) in enumerate(order):
        copies[i].wait()
        out = far if other else near
        out[lax.rem(y + k, 4)] = halves_added(dot(left_terms[...], held[i]))


def right_blocks(left_terms, error):
    return call(
        right_blocks_body,
        (on_chip((4, RANK, COLS), F32), on_chip((4, RANK, COLS), F32)),
        10**10,
        12,
        in_specs=[VMEM, HBM],
        out_specs=(VMEM, VMEM),
        scratch_shapes=[pltpu.VMEM((8, ROWS, COLS), BF16), pltpu.SemaphoreType.DMA((8,))],
    )(left_terms, error)


def add_body(a, b, out):
    out[...] = a[...] + b[...]


def add(a, b):
    return call(add_body, on_chip(a.shape, F32), 10**7)(a, b)


def factor_body(gram, left, inverse_out, basis_out):
    lanes = lax.broadcasted_iota(jnp.int32, (8, 2 * RANK), 1)
    subs = lax.broadcasted_iota(jnp.int32, (8, 2 * RANK), 0)
    work = []
    for i in range(8):
        eye = jnp.where(lanes == subs + (RANK + 8 * i), 1.0, 0.0).astype(F32)
        work.append(jnp.where(lanes < RANK, gram[8 * i : 8 * i + 8, :], eye))
    for j in range(RANK - 1):
        t, r = divmod(j, 8)
        row = work[t][r : r + 1, :]
        row = row * (1.0 / row[:, j : j + 1])
        for i in range(t, 8):
            change = work[i][:, j : j + 1] * row
            if i == t:
                change = jnp.where(subs > r, change, 0.0)
            work[i] = work[i] - change
    parts = []
    for i in range(8):
        pivot = jnp.sum(jnp.where(lanes == subs + 8 * i, work[i], 0.0), axis=1, keepdims=True)
        parts.append(work[i][:, RANK:] / jnp.sqrt(pivot))
    inverse = jnp.concatenate(parts, axis=0)
    inverse_out[...] = inverse
    basis_out[...] = dot(inverse, left[...], NN, HIGHEST).T.astype(BF16)


def factor(gram, left):
    return call(
        factor_body, (on_chip((RANK, RANK), F32), on_chip((ROWS, RANK), BF16)), 6 * 10**9
    )(gram, left)


def right_term_body(inverse, half, other, grads, terms, out):
    first = lax.axis_index(CC) == 0
    low = jnp.where(first, half[...], other[...])
    high = jnp.where(first, other[...], half[...])
    acts_left = two_terms(jnp.concatenate([low, high], axis=1))
    total = terms[0] + terms[1] + terms[2] + terms[3]
    total = total + halves_added(dot(acts_left, grads[...]))
    right = dot(inverse[...], total, NN, HIGHEST)
    for j in range(6):
        for r in range(4):
            out[4 * j + r] = right[16 * r : 16 * r + 16, 128 * j : 128 * j + 128].astype(out.dtype)
    out[24:] = jnp.zeros((8, 16, 128), out.dtype)


def right_term(inverse, half, other, grads, terms):
    return call(right_term_body, on_chip((WORKERS, 16, 128), BF16), 10**8)(
        inverse, half, other, grads, terms
    )


def copies_of_grads(pieces, place, sems):
    own, up, half_a, half_b, down = pieces
    h = TOK // 2
    return [
        [pltpu.make_async_copy(own, place.at[0], sems.at[0])],
        [pltpu.make_async_copy(up, place.at[1], sems.at[1])],
        [
            pltpu.make_async_copy(half_a, place.at[2, pl.ds(0, h)], sems.at[2]),
            pltpu.make_async_copy(half_b, place.at[2, pl.ds(h, h)], sems.at[3]),
        ],
        [pltpu.make_async_copy(down, place.at[3], sems.at[4])],
    ]


def fed_body(acts, error, *rest):
    grads, out, held, held_e, held_o, sems, near_sems, far_sems = rest[:10], *rest[10:]
    errors = [
        pltpu.make_async_copy(
            error.at[:, columns(block_at(k % 4, k >= 4))], held_e.at[k], sems.at[k]
        )
        for k in range(8)
    ]
    loads = copies_of_grads(grads[:5], held.at[pl.ds(0, 4)], near_sems)
    loads += copies_of_grads(grads[5:], held.at[pl.ds(4, 4)], far_sems)
    for k in range(8):
        for c in loads[k]:
            c.start()
        errors[k].start()
    turned = acts[...].T
    stores = []
    for k in range(8):
        for c in loads[k]:
            c.wait()
        errors[k].wait()
        held_o[k] = (dot(turned, held[k]) + held_e[k].astype(F32)).astype(BF16)
        store = pltpu.make_async_copy(held_o.at[k], out.at[k], sems.at[8 + k])
        store.start()
        stores.append(store)
    for store in stores:
        store.wait()


def fed_of(acts, error, grads):
    return call(
        fed_body,
        pltpu.HBM((8, ROWS, COLS), BF16),
        6 * 10**9,
        24,
        in_specs=[VMEM, HBM] + [HBM] * 10,
        out_specs=HBM,
        scratch_shapes=[
            pltpu.VMEM((8, TOK, COLS), BF16),
            pltpu.VMEM((8, ROWS, COLS), BF16),
            pltpu.VMEM((8, ROWS, COLS), BF16),
            pltpu.SemaphoreType.DMA((16,)),
            pltpu.SemaphoreType.DMA((5,)),
            pltpu.SemaphoreType.DMA((5,)),
        ],
    )(acts, error, *map(in_hbm, grads))


def joined(tiles):
    rows = [jnp.concatenate([tiles[4 * j + r] for j in range(6)], axis=1) for r in range(4)]
    return jnp.concatenate(rows, axis=0)


def block_outputs(fed, first, basis, blocks, error_new, sketch_t, held, sems):
    stores = []
    scaled = (basis[...].astype(F32) * (1 / WORKERS)).astype(BF16)
    for i, tiles in enumerate(blocks):
        k = first + i
        where = block_at(k % 4, k >= 4)
        block = joined(tiles)
        held[i] = (fed[i].astype(F32) - dot(scaled, block)).astype(BF16)
        store = pltpu.make_async_copy(held.at[i], error_new.at[0, :, columns(where)], sems.at[i])
        store.start()
        stores.append(store)
        sketch_t[:, columns(where)] = block
    return stores


def own_outputs_body(
    fed, basis, b0, error_new, sketch_t, fed_near, fed_far, held_f, held, sems, load_sems
):
    places = [held_f.at[0]] + [fed_near.at[k] for k in range(3)] + [fed_far.at[k] for k in range(4)]
    loads = [
        pltpu.make_async_copy(fed.at[k], places[k], load_sems.at[k]) for k in range(8)
    ]
    for c in loads:
        c.start()
    loads[0].wait()
    stores = block_outputs(held_f, 0, basis, (b0,), error_new, sketch_t, held, sems)
    for c in loads[1:] + stores:
        c.wait()


def own_outputs(fed, basis, b0):
    return call(
        own_outputs_body,
        (
            sds((1, ROWS, D), BF16),
            on_chip((RANK, D), BF16),
            on_chip((3, ROWS, COLS), BF16),
            on_chip((4, ROWS, COLS), BF16),
        ),
        10**9,
        8,
        in_specs=[HBM, VMEM, VMEM],
        out_specs=(HBM, VMEM, VMEM, VMEM),
        scratch_shapes=[
            pltpu.VMEM((1, ROWS, COLS), BF16),
            pltpu.VMEM((1, ROWS, COLS), BF16),
            pltpu.SemaphoreType.DMA((1,)),
            pltpu.SemaphoreType.DMA((8,)),
        ],
    )(fed, basis, b0)


def near_outputs_body(fed, basis, b1, b2, b3, _, own_t, error_new, sketch_t, held, sems):
    place = columns(block_at(0, False))
    sketch_t[:, place] = own_t[:, place]
    stores = block_outputs(fed, 1, basis, (b1, b2, b3), error_new, sketch_t, held, sems)
    for c in stores:
        c.wait()


def near_outputs(fed_near, basis, blocks, error_new, own_t):
    return call(
        near_outputs_body,
        (sds((1, ROWS, D), BF16), on_chip((RANK, D), BF16)),
        10**9,
        8,
        in_specs=[VMEM] * 5 + [HBM, VMEM],
        out_specs=(HBM, VMEM),
        scratch_shapes=[pltpu.VMEM((3, ROWS, COLS), BF16), pltpu.SemaphoreType.DMA((3,))],
        input_output_aliases={5: 0},
    )(fed_near, basis, *blocks, error_new, own_t)


def far_outputs_body(
    fed, basis, b0, b1, b2, b3, momentum_t, _, near_t, error_new, momentum_new_t, sketch_t, held, sems
):
    for k in range(4):
        place = columns(block_at(k, False))
        sketch_t[:, place] = near_t[:, place]
    stores = block_outputs(fed, 4, basis, (b0, b1, b2, b3), error_new, sketch_t, held, sems)
    w = lax.axis_index(DP)
    quarter = lax.rem(w, 4)
    own = sketch_t[:, columns(w // 4)]
    part = own[:, 0:192]
    for i in (1, 2, 3):
        part = jnp.where(quarter == i, own[:, 192 * i : 192 * (i + 1)], part)
    part = part.astype(F32).T.astype(BF16)
    momentum_new_t[...] = BETA * momentum_t[...] + dot(part, basis[...], NT)
    for store in stores:
        store.wait()


def far_outputs(fed_far, basis, blocks, momentum_t, error_new, near_t):
    return call(
        far_outputs_body,
        (sds((1, ROWS, D), BF16), sds((192, ROWS), F32), sds((RANK, D), BF16)),
        10**9,
        12,
        in_specs=[VMEM] * 7 + [HBM, VMEM],
        out_specs=(HBM, VMEM, VMEM),
        scratch_shapes=[pltpu.VMEM((4, ROWS, COLS), BF16), pltpu.SemaphoreType.DMA((4,))],
        input_output_aliases={7: 0},
    )(fed_far, basis, *blocks, momentum_t, error_new, near_t)


def along_y(x, k):
    return lax.ppermute(x, YY, [(i, (i + k) % 4) for i in range(4)])


def other_core(x):
    return lax.ppermute(x, CC, [(0, 1), (1, 0)])


def to_workers(x):
    return lax.all_to_all(x, DP, split_axis=0, concat_axis=0, tiled=True)


def in_hbm(x):
    return pltpu.with_memory_space_constraint(x, pltpu.HBM)


def after(x, *others):
    return lax.optimization_barrier((x, *others))[0]


def step(activations, out_grads, error, sketch, momentum):
    own_error = in_hbm(error[0])
    sketch_t = in_hbm(sketch.T)
    own_grads, out_grads = out_grads, in_hbm(out_grads)

    mine = grads_sketch(out_grads, sketch_t)
    pair, rounded = pair_sum(mine, other_core(mine))
    others = []
    for k in (1, 2, 3):
        others.append(along_y(rounded, k))
    from_error = error_sketch(own_error, sketch_t)
    tiles = left_term(pair, others, activations, from_error)

    held = after(own_grads, *others)
    g1 = along_y(held, -1)
    g3 = along_y(held, 1)

    arrived = to_workers(tiles)
    copies = sum_and_copy(arrived, F32)
    tiles = to_workers(copies)

    left, left_terms, small, theirs = left_products(tiles, activations)
    other_small = other_core(theirs)
    far, near = right_blocks(left_terms, own_error)
    got = other_core(far)
    small_parts = []
    small = add(small, other_small)
    for k in (1, 2, 3):
        small_parts.append(along_y(small, k))
    q = add(near, got)
    terms = lax.all_to_all(q, YY, split_axis=0, concat_axis=0, tiled=True)
    acts_left, gram = small_sum(small, small_parts)
    acts_left_other = other_core(acts_left)
    inverse, basis = factor(gram, left)
    pieces = right_term(inverse, acts_left, acts_left_other, own_grads, terms)

    half = TOK // 2
    g2a = along_y(after(g1, pieces)[:half], -1)
    g2b = along_y(after(g3, pieces)[half:], 1)
    near_g = (own_grads, g1, g2a, g2b, g3)
    far_g = []
    for k in range(5):
        far_g.append(other_core(after(near_g[k], pieces)))
    arrived = to_workers(pieces)
    copies = sum_and_copy(arrived, BF16)
    fed = fed_of(activations, own_error, (*near_g, *far_g))
    block = to_workers(copies)[:24]
    spread = []
    for k in (1, 2, 3):
        spread.append(along_y(block, -k % 4))
    near_n = (block, *spread)
    far_n = []
    for k in range(4):
        far_n.append(other_core(near_n[k]))
    error_new, own_t, fed_near, fed_far = own_outputs(in_hbm(fed), basis, block)
    error_new, near_t = near_outputs(fed_near, basis, spread, error_new, own_t)
    error_new, momentum_t, sketch_t = far_outputs(
        fed_far, basis, far_n, momentum.T, error_new, near_t
    )
    return error_new, momentum_t.T, sketch_t.T


def solution(mesh):
    split = Mesh(mesh.devices.reshape(8, 4, 4, 2), (*DP, YY, CC))
    mp = (YY, CC)
    return jax.shard_map(
        step,
        mesh=split,
        in_specs=(P(DP, mp), P(DP, mp), P(DP, mp, None), P(), P(mp, DP)),
        out_specs=(P(DP, mp, None), P(mp, DP), P()),
        check_vma=False,
    )
```
